32 devices in a mesh: fsdp: 8 (over z, x), rep: 4 (over y, core).
Axes of the slice: x: 2, y: 2, z: 4, core: 2. Of those that a mesh axis runs over, the one named last changes fastest.
Arguments:
- partials: bfloat16 [4, 56, 1024, 1024], P('rep', None, 'fsdp'), may hold values from -400 to 400
- sketch: bfloat16 [8, 4, 2, 1024, 256], P('fsdp', 'rep'), may hold values from -3 to 3
- owner_table: int32 [56, 1], replicated, may hold values from 0 to 7; in each aligned block of 14 rows (0 to 13, 14 to 27, ...) at most 2 rows name the same one
Outputs:
- update: bfloat16 [56, 1024, 1024], P('rep', 'fsdp')
- new_sketch: bfloat16 [8, 4, 2, 1024, 256], P('fsdp', 'rep')
The draws below stay inside these ranges and needn't reach their ends.
Inputs may be any that keep to these rules, and one draw needn't show every extreme that they name: `owner_table`: in each aligned slice of 14 blocks no owner holds more than 2 blocks; some owner holds exactly 2 in some slice.
All inputs are finite; a program needn't handle non-finite values.
Results may differ from the reference program's by a relative error of at most 0.015.
Values may be sent and summed in bfloat16 or wider, within the bound.
A program may use at most 128 MiB of HBM per device.

```python
import math
import jax
import jax.numpy as jnp
import numpy as np
from jax import lax

BS = 1024
RANK = 256
SLOTS = 2
NS_ITERS = 5
BLK_REP = 14
NB = 56
N_FSDP = 8
N_REP = 4


def draw_partials(key, part):
    row_key, column_key, noise_key = jax.random.split(key, 3)
    row_scale = jnp.exp(jax.random.uniform(row_key, (NB, BS, 1), jnp.float32) * math.log(10.0))
    column_scale = jnp.exp(jax.random.uniform(column_key, (NB, 1, BS), jnp.float32) * math.log(10.0))
    block_place = jnp.arange(NB, dtype=jnp.float32) / NB
    row_place = jnp.arange(BS, dtype=jnp.float32) / BS
    trend = jnp.exp(0.5 * math.log(3.0) * (block_place[:, None, None] + row_place[None, :, None]))
    amplitude = 0.1 * row_scale * column_scale * trend

    def replica(number):
        noise = jnp.clip(jax.random.normal(jax.random.fold_in(noise_key, number), (NB, BS, BS), jnp.float32), -6.0, 6.0)
        return (amplitude * noise).astype(jnp.bfloat16)
    return lax.map(replica, jnp.arange(N_REP, dtype=jnp.int32))


def steps_of(stream_key, dims, shards, smallest, top_value):
    level, own = 1.0, jax.random.fold_in(stream_key, 6)
    for axis_at, shards_of in shards:
        steps = jnp.exp(jax.random.uniform(jax.random.fold_in(own, axis_at), (shards_of,), jnp.float32, smallest / len(shards), top_value / len(shards)))
        level = level * jnp.repeat(steps, dims[axis_at] // shards_of).reshape([-1 if axis == axis_at else 1 for axis in range(len(dims))])
    return level


def assign_block(own_key, own, number, rows, number_of, top, bound, slope):
    ranking = jax.random.permutation(own_key, number_of)
    heavy_load, ordinary = load_shares(number_of, rows * top, bound, slope, True), load_shares(number_of, rows * top, bound, slope, False)
    places = jnp.arange(number_of)

    def named(lengths, offset_by):
        used = int((lengths > 0).sum())
        fixed = max(1, used // 4)
        shifted = fixed + (places - fixed + offset_by * (used - fixed)) % max(1, number_of - fixed)
        return jnp.zeros((number_of,), jnp.int32).at[ranking[jnp.where(places < fixed, places, shifted)]].set(jnp.asarray(lengths, jnp.int32))

    lengths = jnp.where(number % 4 == 0, named(heavy_load, number // 4), named(ordinary, number - number // 4 - 1))
    mixed = jax.random.permutation(jax.random.fold_in(own, 3), number_of)
    giver, taker = mixed[0:number_of // 2 * 2:2], mixed[1:number_of // 2 * 2:2]
    slack = jnp.minimum(lengths[giver] - 1, bound - lengths[taker]) // 2
    slack = jnp.where((giver == ranking[0]) | (taker == ranking[0]) | (lengths[taker] == 0), 0, jnp.maximum(slack, 0))
    shifted = jax.random.randint(jax.random.fold_in(own, 4), (number_of // 2,), 0, 1 << 20) % (slack + 1)
    lengths = lengths.at[giver].add(-shifted).at[taker].add(shifted)
    labels = jnp.searchsorted(jnp.cumsum(lengths), jnp.arange(rows * top), side="right").astype(jnp.int32)
    grid = labels.reshape(top, rows).T
    grid = grid[jax.random.permutation(jax.random.fold_in(own, 1), rows)]
    offset_by = jax.random.randint(jax.random.fold_in(own, 2), (rows, 1), 0, top)
    return jnp.take_along_axis(grid, (jnp.arange(top)[None, :] + offset_by) % top, axis=1)


def load_shares(amount, total, reach, slope, full):
    portions = [(1 << 20) // math.isqrt(standing ** slope) + 1 for standing in range(1, amount + 1)]
    largest = reach if full else min(reach, max(-(-total // amount), total * portions[0] // sum(portions)))
    least = 1 if total - largest >= amount - 1 else 0
    holding, rest = [largest] + [least] * (amount - 1), total - largest - least * (amount - 1)
    while rest > 0:
        movable = [i for i in range(1, amount) if holding[i] < largest] or [i for i in range(1, amount) if holding[i] < reach]
        mass, remaining = sum([portions[i] for i in movable]), rest
        for i in movable:
            extra = min(reach - holding[i], max(1, remaining * portions[i] // mass), rest)
            holding[i] = holding[i] + extra
            rest = rest - extra
    return np.array(holding)


def bell_draw(own_key, shape, scale, most, cuts=(), kind=jnp.bfloat16):
    factor_of = steps_of(own_key, shape, cuts, -0.22, 0.18) if cuts else 1.0
    array = jax.random.normal(own_key, shape, jnp.float32) * scale * factor_of
    return jnp.minimum(jnp.maximum(array, -most), most).astype(kind)


def setup_inputs(seed: int = 0) -> dict:
    seeds = jax.random.split(jax.random.key(seed), 4)
    partials = draw_partials(jax.random.fold_in(seeds[3], 71), 0)
    sketch = bell_draw(seeds[1], (N_FSDP, N_REP, SLOTS, BS, RANK), 0.5, 3.0, ((0, 8), (1, 4)))
    owner_table_keys = jax.random.split(jax.random.fold_in(seeds[2], 1), NB // BLK_REP)
    owner_table_turns = jax.random.permutation(jax.random.fold_in(seeds[2], 3), NB // BLK_REP)
    owner_table = jax.vmap(lambda own, number: assign_block(jax.random.fold_in(seeds[2], 2), own, number, BLK_REP, N_FSDP, 1, SLOTS, 2))(owner_table_keys, owner_table_turns).reshape((NB, 1))
    return {"partials": partials, "sketch": sketch, "owner_table": owner_table}


DECAY = 0.9
DAMPING = 64.0
FIRST_AXES = (((0,), (0,)), ((), ()))
LAST_AXES = (((1,), (1,)), ((), ()))

def inverse_root(matrix, epsilon):
    identity = jnp.eye(matrix.shape[0], dtype=jnp.float32)
    trace_sum = jnp.trace(matrix) + epsilon
    current = matrix / trace_sum
    inverse = identity
    for repeat in range(NS_ITERS):
        middle = 1.5 * identity - 0.5 * jnp.dot(inverse, current, precision=lax.Precision.HIGHEST)
        current = jnp.dot(current, middle, precision=lax.Precision.HIGHEST)
        inverse = jnp.dot(middle, inverse, precision=lax.Precision.HIGHEST)
    return inverse / jnp.sqrt(trace_sum)

def precondition(gradient, current_sketch):
    identity = jnp.eye(current_sketch.shape[1], dtype=jnp.float32)
    projected = lax.dot_general(gradient, current_sketch, FIRST_AXES, preferred_element_type=jnp.float32).astype(jnp.bfloat16)
    gram_matrix = lax.dot_general(current_sketch, current_sketch, FIRST_AXES, preferred_element_type=jnp.float32).astype(jnp.bfloat16)
    powered = DECAY * jnp.dot(current_sketch, gram_matrix, preferred_element_type=jnp.float32) + jnp.dot(gradient, projected, preferred_element_type=jnp.float32)
    inner_gram = lax.dot_general(powered, powered, FIRST_AXES, precision=lax.Precision.HIGHEST)
    basis_full = jnp.dot(powered, inverse_root(inner_gram, 1e-06), precision=lax.Precision.HIGHEST)
    basis_low = basis_full.astype(jnp.bfloat16)
    coefficients = lax.dot_general(gradient, basis_low, FIRST_AXES, preferred_element_type=jnp.float32).astype(jnp.bfloat16)
    alignment = lax.dot_general(current_sketch, basis_low, FIRST_AXES, preferred_element_type=jnp.float32)
    energy = DECAY * lax.dot_general(alignment, alignment, FIRST_AXES, precision=lax.Precision.HIGHEST) + lax.dot_general(coefficients, coefficients, FIRST_AXES, preferred_element_type=jnp.float32)
    root_inverse = inverse_root(energy + DAMPING * identity, 0.0)
    inner_part = jnp.dot(energy, root_inverse, precision=lax.Precision.HIGHEST)
    new_block = jnp.dot(basis_full, inner_part, precision=lax.Precision.HIGHEST).astype(jnp.bfloat16)
    mix_matrix = math.sqrt(DAMPING) * root_inverse - identity
    side_terms = lax.dot_general(coefficients.astype(jnp.float32), mix_matrix, LAST_AXES, precision=lax.Precision.HIGHEST).astype(jnp.bfloat16)
    update_block = (gradient.astype(jnp.float32) + lax.dot_general(basis_low, side_terms, LAST_AXES, preferred_element_type=jnp.float32)).astype(jnp.bfloat16)
    return (update_block, new_block)

def reference(partials, sketch, owner_table):
    owner_ids = owner_table[:, 0]
    block_ids = jnp.arange(NB, dtype=jnp.int32)

    def reduce_block(block):
        replicas = lax.dynamic_index_in_dim(partials, block, axis=1, keepdims=False)
        summed = lax.optimization_barrier(jnp.sum(replicas.astype(jnp.float32), axis=0)).astype(jnp.bfloat16)
        wide = summed.astype(jnp.float32)
        return (summed, jnp.sum(wide * wide))
    gradients, squares = lax.map(reduce_block, block_ids)
    sum_squares = jnp.sum(squares)
    clip_limit = 0.5 * math.sqrt(NB * BS * BS)
    clip_factor = jnp.minimum(1.0, clip_limit / jnp.sqrt(sum_squares + 1e-06))
    slice_ids = block_ids // BLK_REP
    same_owner = (owner_ids[:, None] == owner_ids[None, :]) & (slice_ids[:, None] == slice_ids[None, :]) & (block_ids[:, None] < block_ids[None, :])
    rank_in = lax.optimization_barrier(jnp.sum(same_owner.astype(jnp.int32), axis=0))

    def per_block(block):
        gradient = (clip_factor * gradients[block].astype(jnp.float32)).astype(jnp.bfloat16)
        current_sketch = sketch[owner_ids[block], slice_ids[block], rank_in[block]]
        return precondition(gradient, current_sketch)
    update, fresh_blocks = lax.map(per_block, block_ids)
    new_sketch = sketch.at[owner_ids, slice_ids, rank_in].set(fresh_blocks)
    return (update, new_sketch)
```

```python
import functools
import math

import jax
import jax.numpy as jnp
from jax import lax
from jax.experimental import pallas as pl
from jax.experimental.pallas import tpu as pltpu
from jax.sharding import PartitionSpec as P

NS_ITERS = 5


DECAY = 0.9
DAMPING = 64.0
FIRST_AXES = (((0,), (0,)), ((), ()))
LAST_AXES = (((1,), (1,)), ((), ()))


def inverse_root(matrix, epsilon):
    identity = jnp.eye(matrix.shape[0], dtype=jnp.float32)
    trace_sum = jnp.trace(matrix) + epsilon
    current = matrix / trace_sum
    inverse = identity
    for repeat in range(NS_ITERS):
        middle = 1.5 * identity - 0.5 * jnp.dot(inverse, current, precision=lax.Precision.HIGHEST)
        current = jnp.dot(current, middle, precision=lax.Precision.HIGHEST)
        inverse = jnp.dot(middle, inverse, precision=lax.Precision.HIGHEST)
    return inverse / jnp.sqrt(trace_sum)


def precondition(gradient, current_sketch):
    identity = jnp.eye(current_sketch.shape[1], dtype=jnp.float32)
    projected = lax.dot_general(
        gradient, current_sketch, FIRST_AXES, preferred_element_type=jnp.float32
    ).astype(jnp.bfloat16)
    gram_matrix = lax.dot_general(
        current_sketch, current_sketch, FIRST_AXES, preferred_element_type=jnp.float32
    ).astype(jnp.bfloat16)
    powered = DECAY * jnp.dot(
        current_sketch, gram_matrix, preferred_element_type=jnp.float32
    ) + jnp.dot(gradient, projected, preferred_element_type=jnp.float32)
    inner_gram = lax.dot_general(powered, powered, FIRST_AXES, precision=lax.Precision.HIGHEST)
    basis_full = jnp.dot(powered, inverse_root(inner_gram, 1e-06), precision=lax.Precision.HIGHEST)
    basis_low = basis_full.astype(jnp.bfloat16)
    coefficients = lax.dot_general(
        gradient, basis_low, FIRST_AXES, preferred_element_type=jnp.float32
    ).astype(jnp.bfloat16)
    alignment = lax.dot_general(
        current_sketch, basis_low, FIRST_AXES, preferred_element_type=jnp.float32
    )
    energy = DECAY * lax.dot_general(
        alignment, alignment, FIRST_AXES, precision=lax.Precision.HIGHEST
    ) + lax.dot_general(coefficients, coefficients, FIRST_AXES, preferred_element_type=jnp.float32)
    root_inverse = inverse_root(energy + DAMPING * identity, 0.0)
    inner_part = jnp.dot(energy, root_inverse, precision=lax.Precision.HIGHEST)
    new_block = jnp.dot(basis_full, inner_part, precision=lax.Precision.HIGHEST).astype(
        jnp.bfloat16
    )
    mix_matrix = math.sqrt(DAMPING) * root_inverse - identity
    side_terms = lax.dot_general(
        coefficients.astype(jnp.float32), mix_matrix, LAST_AXES, precision=lax.Precision.HIGHEST
    ).astype(jnp.bfloat16)
    update_block = (
        gradient.astype(jnp.float32)
        + lax.dot_general(basis_low, side_terms, LAST_AXES, preferred_element_type=jnp.float32)
    ).astype(jnp.bfloat16)
    return (update_block, new_block)


def squared_sum(values):
    wide = values.astype(jnp.float32)
    return jnp.sum(wide * wide)


def process_slot(slot_index, arrived, clip_factor, held_sketches, filled):
    block_width = arrived.shape[-1]
    gradient = (clip_factor * arrived.reshape(block_width, block_width).astype(jnp.float32)).astype(
        jnp.bfloat16
    )
    current_sketch = held_sketches[slot_index]
    active = slot_index < filled
    update_block, new_block = precondition(gradient, current_sketch)
    new_block = jnp.where(active, new_block, current_sketch)
    return (update_block, new_block)


def local(partials, sketch, owner_table):
    block_total = partials.shape[1]
    row_count = partials.shape[2]
    block_width = partials.shape[3]
    fsdp_count = lax.axis_size("fsdp")
    per_slice = block_total // lax.axis_size("rep")
    slot_count = sketch.shape[2]
    reduced = lax.psum_scatter(
        partials[0].astype(jnp.float32).astype(jnp.bfloat16), "rep", scatter_dimension=0, tiled=True
    )
    my_owners = lax.dynamic_slice_in_dim(
        owner_table[:, 0], lax.axis_index("rep") * per_slice, per_slice
    )
    positions = jnp.arange(per_slice, dtype=jnp.int32)
    same_owner = (my_owners[:, None] == my_owners[None, :]) & (
        positions[:, None] < positions[None, :]
    )
    rank_in = jnp.sum(same_owner.astype(jnp.int32), axis=0)
    target = rank_in * fsdp_count + my_owners
    selector = (
        target[None, :] == jnp.arange(slot_count * fsdp_count, dtype=jnp.int32)[:, None]
    ).astype(jnp.bfloat16)
    flattened = reduced.reshape(per_slice, row_count * block_width)
    outgoing = jnp.dot(selector, flattened, preferred_element_type=jnp.float32).astype(jnp.bfloat16)
    outgoing = outgoing.reshape(slot_count, fsdp_count, row_count, block_width)
    sum_squares = lax.psum(squared_sum(reduced), ("fsdp", "rep"))
    clip_limit = 0.5 * math.sqrt(block_total * block_width * block_width)
    clip_factor = jnp.minimum(1.0, clip_limit / jnp.sqrt(sum_squares + 1e-06))
    filled = jnp.sum((my_owners == lax.axis_index("fsdp")).astype(jnp.int32))
    held_sketches = sketch[0, 0]
    fresh_list = []
    incoming = lax.all_to_all(outgoing, "fsdp", split_axis=1, concat_axis=1, tiled=True)
    update_list = []
    for slot_index in range(slot_count):
        update_block, new_block = process_slot(
            slot_index, incoming[slot_index], clip_factor, held_sketches, filled
        )
        update_list.append(update_block)
        fresh_list.append(new_block)
    stacked = jnp.stack(update_list).reshape(slot_count, fsdp_count, row_count, block_width)
    returned = lax.all_to_all(stacked, "fsdp", split_axis=1, concat_axis=1, tiled=True)
    returned = returned.reshape(slot_count * fsdp_count, row_count * block_width)
    my_updates = lax.dot_general(
        selector, returned, FIRST_AXES, preferred_element_type=jnp.float32
    ).astype(jnp.bfloat16)
    my_updates = my_updates.reshape(per_slice, row_count, block_width)
    return (my_updates, jnp.stack(fresh_list)[None, None])

MESH = pl.DeviceIdType.MESH
BF = jnp.bfloat16
F32 = jnp.float32


def flip(value, mask, bits):
    result = 0
    for bit in range(bits):
        ours = (value // (1 << bit)) % 2
        theirs = (mask // (1 << bit)) % 2
        result = result + (ours + theirs - 2 * ours * theirs) * (1 << bit)
    return result


def greet(peers):
    barrier = pltpu.get_barrier_semaphore()
    for peer in peers:
        pl.semaphore_signal(barrier, inc=1, device_id=peer, device_id_type=MESH)
    pl.semaphore_wait(barrier, len(peers))


def remote(source, target, send_sem, recv_sem, peer):
    return pltpu.make_async_remote_copy(
        src_ref=source,
        dst_ref=target,
        send_sem=send_sem,
        recv_sem=recv_sem,
        device_id=peer,
        device_id_type=MESH,
    )


def mm(a, b):
    return jnp.dot(a, b, preferred_element_type=F32)


def mm_last(a, b):
    return lax.dot_general(a, b, LAST_AXES, preferred_element_type=F32)


def split(values):
    high = values.astype(BF)
    return high, (values - high.astype(F32)).astype(BF)


def mm3(a, b):
    return mm(a[0], b[0]) + (mm(a[0], b[1]) + mm(a[1], b[0]))


def eye_of(size):
    return (
        lax.broadcasted_iota(jnp.int32, (size, size), 0)
        == lax.broadcasted_iota(jnp.int32, (size, size), 1)
    ).astype(F32)


def kernel_root(matrix, epsilon, identity):
    trace_sum = jnp.sum(matrix * identity, keepdims=True) + epsilon
    current = matrix / trace_sum
    middle = 1.5 * identity - 0.5 * current
    middle_s = split(middle)
    inverse_s = middle_s
    current_s = split(mm3(split(current), middle_s))
    for repeat in range(1, NS_ITERS):
        middle_s = split(1.5 * identity - 0.5 * mm3(inverse_s, current_s))
        if repeat < NS_ITERS - 1:
            current_s = split(mm3(current_s, middle_s))
        inverse = mm3(middle_s, inverse_s)
        inverse_s = split(inverse)
    return inverse / jnp.sqrt(trace_sum)


def step_kernel(
    fsdp, slots, per_slice, clip_limit, owners_ref, sketch_ref, partials_ref, returned_ref, fresh_ref,
    held_0, held_1, held_2, held_3, sketch_held, staged, paired, crossed, totals, summed, incoming, updates, narrow_t, side_t, wide, basis, basis_low,
    square_acc, rep_squares, fsdp_squares, table, scalars,
    load_sems, pair_sems, cross_sems, owner_sems, rep_sems, fsdp_sems, home_sems, self_sems, table_sem,
):
    bits = fsdp.bit_length() - 1
    half = fsdp // 2
    steps = slots * fsdp
    empty = steps - per_slice
    rows = incoming.shape[2]
    width = incoming.shape[3]
    rank = sketch_ref.shape[2]
    tile = rank
    me_f = lax.axis_index("fsdp")
    me_r = lax.axis_index("rep")
    core = me_r % 2
    row = me_r // 2
    partner = row * 2 + 1 - core
    across = (1 - row) * 2 + core
    partner_across = (1 - row) * 2 + 1 - core
    slices = (partner_across, partner, across, me_r)
    held = (held_0, held_1, held_2, held_3)
    loads = [
        pltpu.make_async_copy(
            partials_ref.at[0, pl.ds(number * per_slice, per_slice)], held[n], load_sems.at[n]
        )
        for n, number in enumerate(slices)
    ]
    loads.append(pltpu.make_async_copy(sketch_ref, sketch_held, load_sems.at[len(slices)]))
    for load in loads:
        load.start()
    fill_table(fsdp, slots, per_slice, me_f, owners_ref, table)
    publish = pltpu.make_async_copy(table, scalars, table_sem)
    publish.start()
    greet(
        [{"rep": (me_r + d) % 4} for d in range(1, 4)]
        + [{"fsdp": (me_f + d) % fsdp} for d in range(1, fsdp)]
    )
    square_acc[...] = jnp.zeros_like(square_acc)
    publish.wait()
    loads[0].wait()
    loads[1].wait()

    def block_at(n, k):
        return held[n][scalars[0, slices[n] * per_slice + k]]

    def stage_ref(n, k):
        return updates.at[k // fsdp, k % fsdp] if n == 0 else staged.at[k]

    def pair_copy(n, k):
        return remote(
            stage_ref(n, k), paired.at[n, k], pair_sems.at[0, n, k], pair_sems.at[1, n, k], {"rep": partner}
        )

    def stage(k, carry):
        for n in range(2):
            stage_ref(n, k)[...] = block_at(n, k)
            pair_copy(n, k).start()
        return carry

    lax.fori_loop(0, per_slice, stage, 0)
    for n in range(empty):
        totals[n] = jnp.zeros_like(totals[n])
        totals[empty + per_slice + n] = jnp.zeros_like(totals[n])
    for load in loads[2:]:
        load.wait()

    def where(i):
        place = i % fsdp
        mask = fsdp - 1 - place // 2 - half * (place % 2)
        return i // fsdp, mask, flip(me_f, mask, bits)

    def cross_copy(k):
        return remote(
            paired.at[0, k], crossed.at[k], cross_sems.at[0, k], cross_sems.at[1, k], {"rep": across}
        )

    def owner_copy(i):
        slot, mask, owner = where(i)
        return remote(
            summed.at[i],
            incoming.at[slot, me_f],
            owner_sems.at[0, i],
            owner_sems.at[1, i],
            {"fsdp": owner},
        )

    def send_across(k):
        pair_copy(0, k).wait_recv()
        paired[0, k] = (block_at(2, k).astype(F32) + paired[0, k].astype(F32)).astype(BF)
        cross_copy(k).start()

    def add_up(k):
        pair_copy(1, k).wait_recv()
        pair = block_at(3, k).astype(F32) + paired[1, k].astype(F32)
        cross_copy(k).wait_recv()
        total = (pair + crossed[k].astype(F32)).astype(BF)
        totals[empty + k] = total
        wide_total = total.astype(F32)
        square_acc[...] += jnp.sum((wide_total * wide_total).reshape(rows // 8, 8, width), axis=0)

    def send_owner(i):
        slot, mask, owner = where(i)
        skipped = scalars[1, me_r * steps + i]
        total = totals[empty + i]
        for n in range(1, empty + 1):
            total = jnp.where(skipped == n, totals[empty + i - n], total)

        @pl.when(mask == 0)
        def _():
            incoming[slot, me_f] = total

        @pl.when(mask != 0)
        def _():
            summed[i] = total
            owner_copy(i).start()

    lag = 3

    def first(k, carry):
        send_across(k)
        return carry

    lax.fori_loop(0, lag, first, 0)

    def both(k, carry):
        @pl.when(k < per_slice - lag)
        def _():
            send_across(k + lag)

        add_up(k)
        send_owner(k)
        return carry

    lax.fori_loop(0, per_slice, both, 0)

    def arrived(k):
        def wait_one(n, carry):
            owner_copy(k * fsdp + n).wait_recv()
            return carry

        lax.fori_loop(0, fsdp - 1, wait_one, 0)

    def wide_part(k, part):
        return incoming[k, :, :, part * tile : (part + 1) * tile].reshape(width, tile)

    def project(k, left_t, factor):
        for part in range(width // tile):
            product = mm(left_t, wide_part(k, part))
            if factor is not None:
                product = factor * product
            narrow_t[:, part * tile : (part + 1) * tile] = product.astype(BF)

    lanes = square_acc[:, 0:128]
    for part in range(1, width // 128):
        lanes = lanes + square_acc[:, part * 128 : (part + 1) * 128]
    rep_squares[me_r] = lanes
    rep_copies = [
        remote(
            rep_squares.at[me_r], rep_squares.at[me_r], rep_sems.at[0, d], rep_sems.at[1, d],
            {"rep": (me_r + d) % 4},
        )
        for d in range(1, 4)
    ]
    for copy in rep_copies:
        copy.start()
    arrived(0)
    sketch_t = sketch_held[0].T
    project(0, sketch_t, None)
    for copy in rep_copies:
        copy.wait()
    lanes = rep_squares[0]
    for r in range(1, 4):
        lanes = lanes + rep_squares[r]
    fsdp_squares[me_f] = lanes
    fsdp_copies = [
        remote(
            fsdp_squares.at[me_f], fsdp_squares.at[me_f], fsdp_sems.at[0, d], fsdp_sems.at[1, d],
            {"fsdp": (me_f + d) % fsdp},
        )
        for d in range(1, fsdp)
    ]
    for copy in fsdp_copies:
        copy.start()

    def last(i, carry):
        send_owner(i)
        return carry

    lax.fori_loop(per_slice, steps, last, 0)

    def staged_out(k, carry):
        for n in range(2):
            pair_copy(n, k).wait_send()
        cross_copy(k).wait_send()
        return carry

    lax.fori_loop(0, per_slice, staged_out, 0)
    identity = eye_of(rank)

    def home_copy(k, i):
        home = flip(me_f, fsdp - 1 - i // 2 - half * (i % 2), bits)
        return remote(
            updates.at[k, i], returned_ref.at[k, me_f], home_sems.at[0, k, i], home_sems.at[1, k, i],
            {"fsdp": home},
        )

    def self_copy(k):
        return pltpu.make_async_copy(
            updates.at[k, fsdp - 1], returned_ref.at[k, me_f], self_sems.at[k]
        )

    clip_factor = None
    for k in range(slots):
        sketch = sketch_held[k]
        if k > 0:
            arrived(k)
            sketch_t = sketch.T
            project(k, sketch_t, None)
        gram = mm(sketch_t, sketch).astype(BF)
        projected_t = narrow_t[...]
        for part in range(fsdp):
            span = slice(part * rows, (part + 1) * rows)
            wide[span] = mm_last(incoming[k, part], projected_t)
            basis[span] = DECAY * mm(sketch[span], gram)
        if k == 0:
            for copy in fsdp_copies:
                copy.wait()
            lanes = fsdp_squares[0]
            for f in range(1, fsdp):
                lanes = lanes + fsdp_squares[f]
            sum_squares = jnp.sum(lanes, keepdims=True)
            clip_factor = jnp.minimum(1.0, clip_limit / jnp.sqrt(sum_squares + 1e-06))
        powered_s = split(basis[...] + (clip_factor * clip_factor) * wide[...])
        powered_t = powered_s[0].T
        mixed = mm(powered_t, powered_s[1])
        inner = mm(powered_t, powered_s[0]) + (mixed + mixed.T)
        root = split(kernel_root(inner, 1e-06, identity))
        full = mm3(powered_s, root)
        basis[...] = full
        low = full.astype(BF)
        basis_low[...] = low
        project(k, low.T, clip_factor)
        coefficients_t = narrow_t[...]
        align_s = split(mm(sketch_t, low))
        align_t = (align_s[0].T, align_s[1].T)
        energy = DECAY * mm3(align_t, align_s) + mm_last(coefficients_t, coefficients_t)
        root_inverse = kernel_root(energy + DAMPING * identity, 0.0, identity)
        mix = split(math.sqrt(DAMPING) * root_inverse - identity)
        side_t[...] = (mm(mix[0], coefficients_t) + mm(mix[1], coefficients_t)).astype(BF)

        def send(i, carry):
            home = flip(me_f, fsdp - 1 - i // 2 - half * (i % 2), bits)
            start = pl.multiple_of(home * rows, rows)
            gradient = (clip_factor * incoming[k, home].astype(F32)).astype(BF).astype(F32)
            updates[k, i] = (
                gradient + mm(basis_low[pl.ds(start, rows), :], side_t[...])
            ).astype(BF)

            @pl.when(i == fsdp - 1)
            def _():
                self_copy(k).start()

            @pl.when(i != fsdp - 1)
            def _():
                home_copy(k, i).start()

            return carry

        lax.fori_loop(0, fsdp, send, 0)
        inner_part = split(mm3(split(energy), split(root_inverse)))
        new_block = mm3(split(basis[...]), inner_part).astype(BF)
        active = scalars[2, me_r * steps + k * fsdp + fsdp - 1]
        fresh_ref[k] = jnp.where(active > 0, new_block, sketch)

    def finish(i, carry):
        slot, mask, owner = where(i)

        @pl.when(mask != 0)
        def _():
            owner_copy(i).wait_send()

        return carry

    lax.fori_loop(0, steps, finish, 0)

    def finish_home(i, carry):
        for k in range(slots):
            home_copy(k, i).wait()
        return carry

    lax.fori_loop(0, fsdp - 1, finish_home, 0)
    for k in range(slots):
        self_copy(k).wait()


def fill_table(fsdp, slots, per_slice, me_f, owners_ref, table):
    total = owners_ref.shape[1]
    steps = slots * fsdp
    half = fsdp // 2
    shape = (total, total)
    down = lax.broadcasted_iota(jnp.int32, shape, 0)
    along = lax.broadcasted_iota(jnp.int32, shape, 1)

    def turned(values):
        return jnp.sum(jnp.where(down == along, values, 0), axis=0, keepdims=True)

    owners_along = jnp.broadcast_to(owners_ref[...], shape)
    owners = jnp.sum(jnp.where(down == along, owners_along, 0), axis=1, keepdims=True)
    owners = jnp.broadcast_to(owners, shape)
    same = down // per_slice == along // per_slice
    earlier = same & (owners == owners_along) & (along < down)
    ranks = jnp.sum(jnp.where(earlier, 1, 0), axis=1, keepdims=True)
    mask = lax.bitwise_xor(owners, jnp.full(shape, me_f, jnp.int32))
    place = jnp.where(mask >= half, 2 * (fsdp - 1 - mask), 2 * (half - 1 - mask) + 1)
    spot = jnp.broadcast_to(ranks, shape) * fsdp + place
    ahead = jnp.sum(jnp.where(same & (turned(spot) < spot), 1, 0), axis=1, keepdims=True)
    spots = jnp.max(spot, axis=1, keepdims=True)
    shape = (total, table.shape[1])
    block = lax.broadcasted_iota(jnp.int32, shape, 0)
    lane = lax.broadcasted_iota(jnp.int32, shape, 1)
    group = block // per_slice
    hit = group * per_slice + jnp.broadcast_to(ahead, shape) == lane
    number = jnp.sum(jnp.where(hit, block % per_slice, 0), axis=0, keepdims=True)
    table[0:1, :] = jnp.minimum(number, per_slice - 1)
    ours = group == lane // steps
    spots = jnp.broadcast_to(spots, shape)
    before = jnp.sum(jnp.where(ours & (spots < lane % steps), 1, 0), axis=0, keepdims=True)
    table[1:2, :] = lane[0:1, :] % steps - before
    table[2:3, :] = jnp.sum(jnp.where(ours & (spots == lane % steps), 1, 0), axis=0, keepdims=True)


def place_kernel(fsdp, per_slice, owners_ref, returned_ref, update_ref, held, counts, in_sems, out_sems):
    base = lax.axis_index("rep") * per_slice
    last = returned_ref.shape[0] - 1
    for owner in range(fsdp):
        counts[owner] = 0
    takes, puts = [], []
    for b in range(per_slice):
        owner = owners_ref[base + b]
        count = counts[owner]
        counts[owner] = count + 1
        takes.append(
            pltpu.make_async_copy(returned_ref.at[jnp.minimum(count, last), owner], held.at[b], in_sems.at[b])
        )
        takes[-1].start()
    for b in range(per_slice):
        takes[b].wait()
        puts.append(pltpu.make_async_copy(held.at[b], update_ref.at[b], out_sems.at[b]))
        puts[-1].start()
    for put in puts:
        put.wait()


def fused(partials, sketch, owner_table):
    block_total, rows, width = partials.shape[1:]
    rank = sketch.shape[4]
    fsdp = lax.axis_size("fsdp")
    rep = lax.axis_size("rep")
    slots = sketch.shape[2]
    per_slice = block_total // rep
    steps = slots * fsdp
    table_width = -(-max(rep * steps, block_total) // 128) * 128
    hbm = pl.BlockSpec(memory_space=pl.ANY)
    vmem = pl.BlockSpec(memory_space=pltpu.VMEM)
    smem = pl.BlockSpec(memory_space=pltpu.SMEM)
    dma = pltpu.SemaphoreType.DMA
    block = (rows, width)
    clip_limit = 0.5 * math.sqrt(block_total * width * width)
    returned, fresh = pl.pallas_call(
        functools.partial(step_kernel, fsdp, slots, per_slice, clip_limit),
        out_shape=(
            jax.ShapeDtypeStruct((slots, fsdp) + block, BF),
            jax.ShapeDtypeStruct((slots, width, rank), BF),
        ),
        in_specs=[vmem, hbm, hbm],
        out_specs=(hbm, vmem),
        scratch_shapes=[
            pltpu.VMEM((per_slice,) + block, BF),
            pltpu.VMEM((per_slice,) + block, BF),
            pltpu.VMEM((per_slice,) + block, BF),
            pltpu.VMEM((per_slice,) + block, BF),
            pltpu.VMEM((slots, width, rank), BF),
            pltpu.VMEM((per_slice,) + block, BF),
            pltpu.VMEM((2, per_slice) + block, BF),
            pltpu.VMEM((per_slice,) + block, BF),
            pltpu.VMEM((2 * steps - per_slice,) + block, BF),
            pltpu.VMEM((steps,) + block, BF),
            pltpu.VMEM((slots, fsdp) + block, BF),
            pltpu.VMEM((slots, fsdp) + block, BF),
            pltpu.VMEM((rank, width), BF),
            pltpu.VMEM((rank, width), BF),
            pltpu.VMEM((width, rank), F32),
            pltpu.VMEM((width, rank), F32),
            pltpu.VMEM((width, rank), BF),
            pltpu.VMEM((8, width), F32),
            pltpu.VMEM((rep, 8, 128), F32),
            pltpu.VMEM((fsdp, 8, 128), F32),
            pltpu.VMEM((3, table_width), jnp.int32),
            pltpu.SMEM((3, table_width), jnp.int32),
            dma((rep + 1,)),
            dma((2, 2, per_slice)),
            dma((2, per_slice)),
            dma((2, steps)),
            dma((2, rep)),
            dma((2, fsdp)),
            dma((2, slots, fsdp)),
            dma((slots,)),
            dma,
        ],
        compiler_params=pltpu.CompilerParams(
            collective_id=0, has_side_effects=True, vmem_limit_bytes=VMEM_BYTES
        ),
        name="step",
    )(owner_table.reshape(1, block_total), sketch[0, 0], partials)
    updates = pl.pallas_call(
        functools.partial(place_kernel, fsdp, per_slice),
        out_shape=jax.ShapeDtypeStruct((per_slice,) + block, BF),
        in_specs=[smem, hbm],
        out_specs=hbm,
        scratch_shapes=[
            pltpu.VMEM((per_slice,) + block, BF),
            pltpu.SMEM((fsdp,), jnp.int32),
            dma((per_slice,)),
            dma((per_slice,)),
        ],
        name="place",
    )(owner_table.reshape(block_total), returned)
    return (updates, fresh[None, None])


VMEM_BYTES = 62 * 1024 * 1024


def choose(partials, sketch, owner_table):
    block_total, rows, width = partials.shape[1:]
    fsdp = lax.axis_size("fsdp")
    rep = lax.axis_size("rep")
    steps = sketch.shape[2] * fsdp
    per_slice = block_total // rep
    pairs = rep == 4 and fsdp & (fsdp - 1) == 0 and fsdp >= 4 and 2 * fsdp >= steps >= per_slice > steps - fsdp
    needed = (7 * per_slice + 5 * steps) * rows * width * 2
    if pairs and needed < VMEM_BYTES - (10 << 20):
        return fused(partials, sketch, owner_table)
    return local(partials, sketch, owner_table)


def solution(mesh):
    placed = (P("rep", None, "fsdp", None), P("fsdp", "rep", None, None, None), P())
    return jax.shard_map(
        choose,
        mesh=mesh,
        in_specs=placed,
        out_specs=(P("rep", "fsdp", None), P("fsdp", "rep", None, None, None)),
        check_vma=False,
    )
```

```python
import functools
import math

import jax
import jax.numpy as jnp
from jax import lax
from jax.experimental import pallas as pl
from jax.experimental.pallas import tpu as pltpu
from jax.sharding import PartitionSpec as P

NS_ITERS = 5


DECAY = 0.9
DAMPING = 64.0
FIRST_AXES = (((0,), (0,)), ((), ()))
LAST_AXES = (((1,), (1,)), ((), ()))


def inverse_root(matrix, epsilon):
    identity = jnp.eye(matrix.shape[0], dtype=jnp.float32)
    trace_sum = jnp.trace(matrix) + epsilon
    current = matrix / trace_sum
    inverse = identity
    for repeat in range(NS_ITERS):
        middle = 1.5 * identity - 0.5 * jnp.dot(inverse, current, precision=lax.Precision.HIGHEST)
        current = jnp.dot(current, middle, precision=lax.Precision.HIGHEST)
        inverse = jnp.dot(middle, inverse, precision=lax.Precision.HIGHEST)
    return inverse / jnp.sqrt(trace_sum)


def precondition(gradient, current_sketch):
    identity = jnp.eye(current_sketch.shape[1], dtype=jnp.float32)
    projected = lax.dot_general(
        gradient, current_sketch, FIRST_AXES, preferred_element_type=jnp.float32
    ).astype(jnp.bfloat16)
    gram_matrix = lax.dot_general(
        current_sketch, current_sketch, FIRST_AXES, preferred_element_type=jnp.float32
    ).astype(jnp.bfloat16)
    powered = DECAY * jnp.dot(
        current_sketch, gram_matrix, preferred_element_type=jnp.float32
    ) + jnp.dot(gradient, projected, preferred_element_type=jnp.float32)
    inner_gram = lax.dot_general(powered, powered, FIRST_AXES, precision=lax.Precision.HIGHEST)
    basis_full = jnp.dot(powered, inverse_root(inner_gram, 1e-06), precision=lax.Precision.HIGHEST)
    basis_low = basis_full.astype(jnp.bfloat16)
    coefficients = lax.dot_general(
        gradient, basis_low, FIRST_AXES, preferred_element_type=jnp.float32
    ).astype(jnp.bfloat16)
    alignment = lax.dot_general(
        current_sketch, basis_low, FIRST_AXES, preferred_element_type=jnp.float32
    )
    energy = DECAY * lax.dot_general(
        alignment, alignment, FIRST_AXES, precision=lax.Precision.HIGHEST
    ) + lax.dot_general(coefficients, coefficients, FIRST_AXES, preferred_element_type=jnp.float32)
    root_inverse = inverse_root(energy + DAMPING * identity, 0.0)
    inner_part = jnp.dot(energy, root_inverse, precision=lax.Precision.HIGHEST)
    new_block = jnp.dot(basis_full, inner_part, precision=lax.Precision.HIGHEST).astype(
        jnp.bfloat16
    )
    mix_matrix = math.sqrt(DAMPING) * root_inverse - identity
    side_terms = lax.dot_general(
        coefficients.astype(jnp.float32), mix_matrix, LAST_AXES, precision=lax.Precision.HIGHEST
    ).astype(jnp.bfloat16)
    update_block = (
        gradient.astype(jnp.float32)
        + lax.dot_general(basis_low, side_terms, LAST_AXES, preferred_element_type=jnp.float32)
    ).astype(jnp.bfloat16)
    return (update_block, new_block)


def squared_sum(values):
    wide = values.astype(jnp.float32)
    return jnp.sum(wide * wide)


def process_slot(slot_index, arrived, clip_factor, held_sketches, filled):
    block_width = arrived.shape[-1]
    gradient = (clip_factor * arrived.reshape(block_width, block_width).astype(jnp.float32)).astype(
        jnp.bfloat16
    )
    current_sketch = held_sketches[slot_index]
    active = slot_index < filled
    update_block, new_block = precondition(gradient, current_sketch)
    new_block = jnp.where(active, new_block, current_sketch)
    return (update_block, new_block)


def local(partials, sketch, owner_table):
    block_total = partials.shape[1]
    row_count = partials.shape[2]
    block_width = partials.shape[3]
    fsdp_count = lax.axis_size("fsdp")
    per_slice = block_total // lax.axis_size("rep")
    slot_count = sketch.shape[2]
    reduced = lax.psum_scatter(
        partials[0].astype(jnp.float32).astype(jnp.bfloat16), "rep", scatter_dimension=0, tiled=True
    )
    my_owners = lax.dynamic_slice_in_dim(
        owner_table[:, 0], lax.axis_index("rep") * per_slice, per_slice
    )
    positions = jnp.arange(per_slice, dtype=jnp.int32)
    same_owner = (my_owners[:, None] == my_owners[None, :]) & (
        positions[:, None] < positions[None, :]
    )
    rank_in = jnp.sum(same_owner.astype(jnp.int32), axis=0)
    target = rank_in * fsdp_count + my_owners
    selector = (
        target[None, :] == jnp.arange(slot_count * fsdp_count, dtype=jnp.int32)[:, None]
    ).astype(jnp.bfloat16)
    flattened = reduced.reshape(per_slice, row_count * block_width)
    outgoing = jnp.dot(selector, flattened, preferred_element_type=jnp.float32).astype(jnp.bfloat16)
    outgoing = outgoing.reshape(slot_count, fsdp_count, row_count, block_width)
    sum_squares = lax.psum(squared_sum(reduced), ("fsdp", "rep"))
    clip_limit = 0.5 * math.sqrt(block_total * block_width * block_width)
    clip_factor = jnp.minimum(1.0, clip_limit / jnp.sqrt(sum_squares + 1e-06))
    filled = jnp.sum((my_owners == lax.axis_index("fsdp")).astype(jnp.int32))
    held_sketches = sketch[0, 0]
    fresh_list = []
    incoming = lax.all_to_all(outgoing, "fsdp", split_axis=1, concat_axis=1, tiled=True)
    update_list = []
    for slot_index in range(slot_count):
        update_block, new_block = process_slot(
            slot_index, incoming[slot_index], clip_factor, held_sketches, filled
        )
        update_list.append(update_block)
        fresh_list.append(new_block)
    stacked = jnp.stack(update_list).reshape(slot_count, fsdp_count, row_count, block_width)
    returned = lax.all_to_all(stacked, "fsdp", split_axis=1, concat_axis=1, tiled=True)
    returned = returned.reshape(slot_count * fsdp_count, row_count * block_width)
    my_updates = lax.dot_general(
        selector, returned, FIRST_AXES, preferred_element_type=jnp.float32
    ).astype(jnp.bfloat16)
    my_updates = my_updates.reshape(per_slice, row_count, block_width)
    return (my_updates, jnp.stack(fresh_list)[None, None])

MESH = pl.DeviceIdType.MESH
BF = jnp.bfloat16
F32 = jnp.float32


def flip(value, mask, bits):
    result = 0
    for bit in range(bits):
        ours = (value // (1 << bit)) % 2
        theirs = (mask // (1 << bit)) % 2
        result = result + (ours + theirs - 2 * ours * theirs) * (1 << bit)
    return result


def greet(peers):
    barrier = pltpu.get_barrier_semaphore()
    for peer in peers:
        pl.semaphore_signal(barrier, inc=1, device_id=peer, device_id_type=MESH)
    pl.semaphore_wait(barrier, len(peers))


def remote(source, target, send_sem, recv_sem, peer):
    return pltpu.make_async_remote_copy(
        src_ref=source,
        dst_ref=target,
        send_sem=send_sem,
        recv_sem=recv_sem,
        device_id=peer,
        device_id_type=MESH,
    )


def mm(a, b):
    return jnp.dot(a, b, preferred_element_type=F32)


def mm_last(a, b):
    return lax.dot_general(a, b, LAST_AXES, preferred_element_type=F32)


def split(values):
    high = values.astype(BF)
    return high, (values - high.astype(F32)).astype(BF)


def mm3(a, b):
    return mm(a[0], b[0]) + (mm(a[0], b[1]) + mm(a[1], b[0]))


def eye_of(size):
    return (
        lax.broadcasted_iota(jnp.int32, (size, size), 0)
        == lax.broadcasted_iota(jnp.int32, (size, size), 1)
    ).astype(F32)


def kernel_root(matrix, epsilon, identity):
    trace_sum = jnp.sum(matrix * identity, keepdims=True) + epsilon
    current = matrix / trace_sum
    middle = 1.5 * identity - 0.5 * current
    middle_s = split(middle)
    inverse_s = middle_s
    current_s = split(mm3(split(current), middle_s))
    for repeat in range(1, NS_ITERS):
        middle_s = split(1.5 * identity - 0.5 * mm3(inverse_s, current_s))
        if repeat < NS_ITERS - 1:
            current_s = split(mm3(current_s, middle_s))
        inverse = mm3(middle_s, inverse_s)
        inverse_s = split(inverse)
    return inverse / jnp.sqrt(trace_sum)


def step_kernel(
    fsdp, slots, per_slice, clip_limit, owners_ref, sketch_ref, partials_ref, returned_ref, fresh_ref,
    held_0, held_1, held_2, held_3, sketch_held, staged, paired, crossed, totals, summed, incoming, updates, landing, factor_in, basis_in, narrow_t, side_t, wide, basis, basis_low,
    square_acc, rep_squares, fsdp_squares, table, scalars,
    load_sems, pair_sems, cross_sems, owner_sems, rep_sems, fsdp_sems, home_sems, self_sems, table_sem,
    basis_sends, basis_recvs, factor_sends, factor_recvs, land_sends, land_recvs, far_sems,
):
    bits = fsdp.bit_length() - 1
    half = fsdp // 2
    steps = slots * fsdp
    empty = steps - per_slice
    rows = incoming.shape[2]
    width = incoming.shape[3]
    rank = sketch_ref.shape[2]
    tile = rank
    me_f = lax.axis_index("fsdp")
    me_r = lax.axis_index("rep")
    core = me_r % 2
    row = me_r // 2
    partner = row * 2 + 1 - core
    across = (1 - row) * 2 + core
    partner_across = (1 - row) * 2 + 1 - core
    slices = (partner_across, partner, across, me_r)
    held = (held_0, held_1, held_2, held_3)
    loads = [
        pltpu.make_async_copy(
            partials_ref.at[0, pl.ds(number * per_slice, per_slice)], held[n], load_sems.at[n]
        )
        for n, number in enumerate(slices)
    ]
    loads.append(pltpu.make_async_copy(sketch_ref, sketch_held, load_sems.at[len(slices)]))
    for load in loads:
        load.start()
    fill_table(fsdp, slots, per_slice, me_f, owners_ref, table)
    publish = pltpu.make_async_copy(table, scalars, table_sem)
    publish.start()
    greet(
        [{"rep": (me_r + d) % 4} for d in range(1, 4)]
        + [{"fsdp": (me_f + d) % fsdp} for d in range(1, fsdp)]
    )
    square_acc[...] = jnp.zeros_like(square_acc)
    publish.wait()
    loads[0].wait()
    loads[1].wait()

    def block_at(n, k):
        return held[n][scalars[0, slices[n] * per_slice + k]]

    def stage_ref(n, k):
        return updates.at[k // fsdp, k % fsdp] if n == 0 else staged.at[k]

    def pair_copy(n, k):
        return remote(
            stage_ref(n, k), paired.at[n, k], pair_sems.at[0, n, k], pair_sems.at[1, n, k], {"rep": partner}
        )

    def stage(k, carry):
        for n in range(2):
            stage_ref(n, k)[...] = block_at(n, k)
            pair_copy(n, k).start()
        return carry

    lax.fori_loop(0, per_slice, stage, 0)
    for n in range(empty):
        totals[n] = jnp.zeros_like(totals[n])
        totals[empty + per_slice + n] = jnp.zeros_like(totals[n])
    for load in loads[2:]:
        load.wait()

    def where(i):
        place = i % fsdp
        mask = fsdp - 1 - place // 2 - half * (place % 2)
        return i // fsdp, mask, flip(me_f, mask, bits)

    def cross_copy(k):
        return remote(
            paired.at[0, k], crossed.at[k], cross_sems.at[0, k], cross_sems.at[1, k], {"rep": across}
        )

    def owner_copy(i):
        slot, mask, owner = where(i)
        return remote(
            summed.at[i],
            incoming.at[slot, me_f],
            owner_sems.at[0, i],
            owner_sems.at[1, i],
            {"fsdp": owner},
        )

    def send_across(k):
        pair_copy(0, k).wait_recv()
        paired[0, k] = (block_at(2, k).astype(F32) + paired[0, k].astype(F32)).astype(BF)
        cross_copy(k).start()

    def add_up(k):
        pair_copy(1, k).wait_recv()
        pair = block_at(3, k).astype(F32) + paired[1, k].astype(F32)
        cross_copy(k).wait_recv()
        total = (pair + crossed[k].astype(F32)).astype(BF)
        totals[empty + k] = total
        wide_total = total.astype(F32)
        square_acc[...] += jnp.sum((wide_total * wide_total).reshape(rows // 8, 8, width), axis=0)

    def send_owner(i):
        slot, mask, owner = where(i)
        skipped = scalars[1, me_r * steps + i]
        total = totals[empty + i]
        for n in range(1, empty + 1):
            total = jnp.where(skipped == n, totals[empty + i - n], total)

        @pl.when(mask == 0)
        def _():
            incoming[slot, me_f] = total

        @pl.when(mask != 0)
        def _():
            summed[i] = total
            owner_copy(i).start()

    lag = 3

    def first(k, carry):
        send_across(k)
        return carry

    lax.fori_loop(0, lag, first, 0)

    def both(k, carry):
        @pl.when(k < per_slice - lag)
        def _():
            send_across(k + lag)

        add_up(k)
        send_owner(k)
        return carry

    lax.fori_loop(0, per_slice, both, 0)

    def arrived(k):
        def wait_one(n, carry):
            owner_copy(k * fsdp + n).wait_recv()
            return carry

        lax.fori_loop(0, fsdp - 1, wait_one, 0)

    def wide_part(k, part):
        return incoming[k, :, :, part * tile : (part + 1) * tile].reshape(width, tile)

    def project(k, left_t, factor):
        for part in range(width // tile):
            product = mm(left_t, wide_part(k, part))
            if factor is not None:
                product = factor * product
            narrow_t[:, part * tile : (part + 1) * tile] = product.astype(BF)

    lanes = square_acc[:, 0:128]
    for part in range(1, width // 128):
        lanes = lanes + square_acc[:, part * 128 : (part + 1) * 128]
    rep_squares[me_r] = lanes
    rep_copies = [
        remote(
            rep_squares.at[me_r], rep_squares.at[me_r], rep_sems.at[0, d], rep_sems.at[1, d],
            {"rep": (me_r + d) % 4},
        )
        for d in range(1, 4)
    ]
    for copy in rep_copies:
        copy.start()
    arrived(0)
    sketch_t = sketch_held[0].T
    project(0, sketch_t, None)
    for copy in rep_copies:
        copy.wait()
    lanes = rep_squares[0]
    for r in range(1, 4):
        lanes = lanes + rep_squares[r]
    fsdp_squares[me_f] = lanes
    fsdp_copies = [
        remote(
            fsdp_squares.at[me_f], fsdp_squares.at[me_f], fsdp_sems.at[0, d], fsdp_sems.at[1, d],
            {"fsdp": (me_f + d) % fsdp},
        )
        for d in range(1, fsdp)
    ]
    for copy in fsdp_copies:
        copy.start()

    def last(i, carry):
        send_owner(i)
        return carry

    lax.fori_loop(per_slice, steps, last, 0)

    def staged_out(k, carry):
        for n in range(2):
            pair_copy(n, k).wait_send()
        cross_copy(k).wait_send()
        return carry

    lax.fori_loop(0, per_slice, staged_out, 0)
    identity = eye_of(rank)

    side = me_f % 2
    top = me_f // half
    base = half * top
    other = half - base
    parts = width // tile
    groups = half // 2
    relay = half + side - 2 * top
    is_relay = me_f // 2 == groups - 1 + top

    def columns(p):
        return pl.ds(pl.multiple_of(p * tile, tile), tile)

    def basis_copy(k, group):
        return remote(
            basis_low.at[k, pl.ds(pl.multiple_of(other * rows, rows), half * rows)],
            basis_in.at[k, group],
            basis_sends.at[k],
            basis_recvs.at[k, group],
            {"fsdp": relay},
        )

    def factor_copy(k, group, p):
        return remote(
            side_t.at[k, :, columns(p)],
            factor_in.at[k, group, :, columns(p)],
            factor_sends.at[k, p],
            factor_recvs.at[k, group, p],
            {"fsdp": relay},
        )

    def land_copy(k, group, e, p):
        return remote(
            incoming.at[k, group * half + e, :, columns(p)],
            landing.at[k, 2 * group + side, :, columns(p)],
            land_sends.at[k, group, e, p],
            land_recvs.at[k, 2 * group + side, p],
            {"fsdp": base + e},
        )

    def landed(k, q, p):
        return remote(
            incoming.at[k, q, :, columns(p)],
            landing.at[k, q, :, columns(p)],
            land_sends.at[k, 0, 0, p],
            land_recvs.at[k, q, p],
            {"fsdp": relay},
        )

    def home_copy(k, mask):
        return remote(
            updates.at[k, mask], returned_ref.at[k, me_f], home_sems.at[0, k, mask], home_sems.at[1, k, mask],
            {"fsdp": flip(me_f, mask, bits)},
        )

    def self_copy(k):
        return pltpu.make_async_copy(updates.at[k, 0], returned_ref.at[k, me_f], self_sems.at[k])

    def far_place(m):
        return 2 * (half - 1 - m)

    def far_copy(k, m):
        return pltpu.make_async_copy(
            summed.at[k * fsdp + far_place(m)],
            returned_ref.at[k, flip(me_f, half + m, bits)],
            far_sems.at[k, m],
        )

    def pass_on(k):
        def step(n, carry):
            p = n // groups
            group = n % groups

            @pl.when(p == 0)
            def _():
                basis_copy(k, group).wait_recv()

            factor_copy(k, group, p).wait_recv()
            product = mm(basis_in[k, group], factor_in[k, group, :, columns(p)]).astype(BF)
            for e in range(half):
                piece = product[e * rows : (e + 1) * rows]

                @pl.when(e == me_f - base)
                def _():
                    landing[k, 2 * group + side, :, columns(p)] = piece

                @pl.when(e != me_f - base)
                def _():
                    incoming[k, group * half + e, :, columns(p)] = piece
                    land_copy(k, group, e, p).start()

            return carry

        lax.fori_loop(0, parts * groups, step, 0)

    def combine(k):
        def one(m, carry):
            q = flip(me_f, half + m, bits) - other
            i = k * fsdp + far_place(m)
            owner_copy(i).wait_send()

            @pl.when((q % 2 != side) | (me_f // 2 != groups - 1 + top))
            def _():
                for p in range(parts):
                    landed(k, q, p).wait_recv()

            gradient = (clip_factor * summed[i].astype(F32)).astype(BF).astype(F32)
            summed[i] = (gradient + landing[k, q].astype(F32)).astype(BF)
            far_copy(k, m).start()
            return carry

        lax.fori_loop(0, half, one, 0)

    clip_factor = None
    for k in range(slots):
        sketch = sketch_held[k]
        if k > 0:
            arrived(k)
            sketch_t = sketch.T
            project(k, sketch_t, None)
        gram = mm(sketch_t, sketch).astype(BF)
        projected_t = narrow_t[...]
        for part in range(fsdp):
            span = slice(part * rows, (part + 1) * rows)
            wide[span] = mm_last(incoming[k, part], projected_t)
            basis[span] = DECAY * mm(sketch[span], gram)
        if k == 0:
            for copy in fsdp_copies:
                copy.wait()
            lanes = fsdp_squares[0]
            for f in range(1, fsdp):
                lanes = lanes + fsdp_squares[f]
            sum_squares = jnp.sum(lanes, keepdims=True)
            clip_factor = jnp.minimum(1.0, clip_limit / jnp.sqrt(sum_squares + 1e-06))
        powered_s = split(basis[...] + (clip_factor * clip_factor) * wide[...])
        powered_t = powered_s[0].T
        mixed = mm(powered_t, powered_s[1])
        inner = mm(powered_t, powered_s[0]) + (mixed + mixed.T)
        root = split(kernel_root(inner, 1e-06, identity))
        full = mm3(powered_s, root)
        basis[...] = full
        low = full.astype(BF)
        basis_low[k] = low
        basis_copy(k, me_f % half // 2).start()
        project(k, low.T, clip_factor)
        coefficients_t = narrow_t[...]
        align_s = split(mm(sketch_t, low))
        align_t = (align_s[0].T, align_s[1].T)
        energy = DECAY * mm3(align_t, align_s) + mm_last(coefficients_t, coefficients_t)
        root_inverse = kernel_root(energy + DAMPING * identity, 0.0, identity)
        mix = split(math.sqrt(DAMPING) * root_inverse - identity)
        for part in range(parts):
            span = slice(part * tile, (part + 1) * tile)
            chosen = coefficients_t[:, span]
            side_t[k, :, span] = (mm(mix[0], chosen) + mm(mix[1], chosen)).astype(BF)
            factor_copy(k, me_f % half // 2, part).start()

        def send(i, carry):
            mask = half - 1 - i
            home = flip(me_f, mask, bits)
            start = pl.multiple_of(home * rows, rows)
            gradient = (clip_factor * incoming[k, home].astype(F32)).astype(BF).astype(F32)
            updates[k, mask] = (
                gradient + mm(basis_low[k, pl.ds(start, rows), :], side_t[k])
            ).astype(BF)

            @pl.when(mask == 0)
            def _():
                self_copy(k).start()

            @pl.when(mask != 0)
            def _():
                home_copy(k, mask).start()

            return carry

        lax.fori_loop(0, half, send, 0)
        inner_part = split(mm3(split(energy), split(root_inverse)))
        new_block = mm3(split(basis[...]), inner_part).astype(BF)
        active = scalars[2, me_r * steps + k * fsdp + fsdp - 1]
        fresh_ref[k] = jnp.where(active > 0, new_block, sketch)

    for k in range(slots):

        @pl.when(is_relay)
        def _():
            pass_on(k)

        combine(k)

    def finish(mask, carry):
        for k in range(slots):
            owner_copy(k * fsdp + 2 * (half - 1 - mask) + 1).wait_send()
            home_copy(k, mask).wait()
        return carry

    lax.fori_loop(1, half, finish, 0)

    def finish_parts(p, carry):
        for k in range(slots):
            factor_copy(k, 0, p).wait_send()
        return carry

    lax.fori_loop(0, parts, finish_parts, 0)

    @pl.when(is_relay)
    def _():
        def drain(n, carry):
            group = n // (half * parts)
            e = n // parts % half

            @pl.when(e != me_f - base)
            def _():
                for k in range(slots):
                    land_copy(k, group, e, n % parts).wait_send()

            return carry

        lax.fori_loop(0, groups * half * parts, drain, 0)

    def finish_far(m, carry):
        for k in range(slots):
            far_copy(k, m).wait()
        return carry

    lax.fori_loop(0, half, finish_far, 0)
    for k in range(slots):
        basis_copy(k, 0).wait_send()
        self_copy(k).wait()


def fill_table(fsdp, slots, per_slice, me_f, owners_ref, table):
    total = owners_ref.shape[1]
    steps = slots * fsdp
    half = fsdp // 2
    shape = (total, total)
    down = lax.broadcasted_iota(jnp.int32, shape, 0)
    along = lax.broadcasted_iota(jnp.int32, shape, 1)

    def turned(values):
        return jnp.sum(jnp.where(down == along, values, 0), axis=0, keepdims=True)

    owners_along = jnp.broadcast_to(owners_ref[...], shape)
    owners = jnp.sum(jnp.where(down == along, owners_along, 0), axis=1, keepdims=True)
    owners = jnp.broadcast_to(owners, shape)
    same = down // per_slice == along // per_slice
    earlier = same & (owners == owners_along) & (along < down)
    ranks = jnp.sum(jnp.where(earlier, 1, 0), axis=1, keepdims=True)
    mask = lax.bitwise_xor(owners, jnp.full(shape, me_f, jnp.int32))
    place = jnp.where(mask >= half, 2 * (fsdp - 1 - mask), 2 * (half - 1 - mask) + 1)
    spot = jnp.broadcast_to(ranks, shape) * fsdp + place
    ahead = jnp.sum(jnp.where(same & (turned(spot) < spot), 1, 0), axis=1, keepdims=True)
    spots = jnp.max(spot, axis=1, keepdims=True)
    shape = (total, table.shape[1])
    block = lax.broadcasted_iota(jnp.int32, shape, 0)
    lane = lax.broadcasted_iota(jnp.int32, shape, 1)
    group = block // per_slice
    hit = group * per_slice + jnp.broadcast_to(ahead, shape) == lane
    number = jnp.sum(jnp.where(hit, block % per_slice, 0), axis=0, keepdims=True)
    table[0:1, :] = jnp.minimum(number, per_slice - 1)
    ours = group == lane // steps
    spots = jnp.broadcast_to(spots, shape)
    before = jnp.sum(jnp.where(ours & (spots < lane % steps), 1, 0), axis=0, keepdims=True)
    table[1:2, :] = lane[0:1, :] % steps - before
    table[2:3, :] = jnp.sum(jnp.where(ours & (spots == lane % steps), 1, 0), axis=0, keepdims=True)


def place_kernel(fsdp, per_slice, owners_ref, returned_ref, update_ref, held, counts, in_sems, out_sems):
    base = lax.axis_index("rep") * per_slice
    last = returned_ref.shape[0] - 1
    for owner in range(fsdp):
        counts[owner] = 0
    takes, puts = [], []
    for b in range(per_slice):
        owner = owners_ref[base + b]
        count = counts[owner]
        counts[owner] = count + 1
        takes.append(
            pltpu.make_async_copy(returned_ref.at[jnp.minimum(count, last), owner], held.at[b], in_sems.at[b])
        )
        takes[-1].start()
    for b in range(per_slice):
        takes[b].wait()
        puts.append(pltpu.make_async_copy(held.at[b], update_ref.at[b], out_sems.at[b]))
        puts[-1].start()
    for put in puts:
        put.wait()


def fused(partials, sketch, owner_table):
    block_total, rows, width = partials.shape[1:]
    rank = sketch.shape[4]
    fsdp = lax.axis_size("fsdp")
    rep = lax.axis_size("rep")
    slots = sketch.shape[2]
    per_slice = block_total // rep
    steps = slots * fsdp
    table_width = -(-max(rep * steps, block_total) // 128) * 128
    hbm = pl.BlockSpec(memory_space=pl.ANY)
    vmem = pl.BlockSpec(memory_space=pltpu.VMEM)
    smem = pl.BlockSpec(memory_space=pltpu.SMEM)
    dma = pltpu.SemaphoreType.DMA
    block = (rows, width)
    half = fsdp // 2
    groups = half // 2
    parts = width // rank
    clip_limit = 0.5 * math.sqrt(block_total * width * width)
    returned, fresh = pl.pallas_call(
        functools.partial(step_kernel, fsdp, slots, per_slice, clip_limit),
        out_shape=(
            jax.ShapeDtypeStruct((slots, fsdp) + block, BF),
            jax.ShapeDtypeStruct((slots, width, rank), BF),
        ),
        in_specs=[vmem, hbm, hbm],
        out_specs=(hbm, vmem),
        scratch_shapes=[
            pltpu.VMEM((per_slice,) + block, BF),
            pltpu.VMEM((per_slice,) + block, BF),
            pltpu.VMEM((per_slice,) + block, BF),
            pltpu.VMEM((per_slice,) + block, BF),
            pltpu.VMEM((slots, width, rank), BF),
            pltpu.VMEM((per_slice,) + block, BF),
            pltpu.VMEM((2, per_slice) + block, BF),
            pltpu.VMEM((per_slice,) + block, BF),
            pltpu.VMEM((2 * steps - per_slice,) + block, BF),
            pltpu.VMEM((steps,) + block, BF),
            pltpu.VMEM((slots, fsdp) + block, BF),
            pltpu.VMEM((slots, fsdp) + block, BF),
            pltpu.VMEM((slots, half) + block, BF),
            pltpu.VMEM((slots, groups, rank, width), BF),
            pltpu.VMEM((slots, groups, half * rows, rank), BF),
            pltpu.VMEM((rank, width), BF),
            pltpu.VMEM((slots, rank, width), BF),
            pltpu.VMEM((width, rank), F32),
            pltpu.VMEM((width, rank), F32),
            pltpu.VMEM((slots, width, rank), BF),
            pltpu.VMEM((8, width), F32),
            pltpu.VMEM((rep, 8, 128), F32),
            pltpu.VMEM((fsdp, 8, 128), F32),
            pltpu.VMEM((3, table_width), jnp.int32),
            pltpu.SMEM((3, table_width), jnp.int32),
            dma((rep + 1,)),
            dma((2, 2, per_slice)),
            dma((2, per_slice)),
            dma((2, steps)),
            dma((2, rep)),
            dma((2, fsdp)),
            dma((2, slots, half)),
            dma((slots,)),
            dma,
            dma((slots,)),
            dma((slots, groups)),
            dma((slots, parts)),
            dma((slots, groups, parts)),
            dma((slots, groups, half, parts)),
            dma((slots, half, parts)),
            dma((slots, half)),
        ],
        compiler_params=pltpu.CompilerParams(
            collective_id=0, has_side_effects=True, vmem_limit_bytes=VMEM_BYTES
        ),
        name="step",
    )(owner_table.reshape(1, block_total), sketch[0, 0], partials)
    updates = pl.pallas_call(
        functools.partial(place_kernel, fsdp, per_slice),
        out_shape=jax.ShapeDtypeStruct((per_slice,) + block, BF),
        in_specs=[smem, hbm],
        out_specs=hbm,
        scratch_shapes=[
            pltpu.VMEM((per_slice,) + block, BF),
            pltpu.SMEM((fsdp,), jnp.int32),
            dma((per_slice,)),
            dma((per_slice,)),
        ],
        name="place",
    )(owner_table.reshape(block_total), returned)
    return (updates, fresh[None, None])


VMEM_BYTES = 62 * 1024 * 1024


def choose(partials, sketch, owner_table):
    block_total, rows, width = partials.shape[1:]
    fsdp = lax.axis_size("fsdp")
    rep = lax.axis_size("rep")
    steps = sketch.shape[2] * fsdp
    per_slice = block_total // rep
    pairs = rep == 4 and fsdp & (fsdp - 1) == 0 and fsdp >= 4 and 2 * fsdp >= steps >= per_slice > steps - fsdp
    needed = (7 * per_slice + 5 * steps) * rows * width * 2
    if pairs and needed < VMEM_BYTES - (10 << 20):
        return fused(partials, sketch, owner_table)
    return local(partials, sketch, owner_table)


def solution(mesh):
    placed = (P("rep", None, "fsdp", None), P("fsdp", "rep", None, None, None), P())
    return jax.shard_map(
        choose,
        mesh=mesh,
        in_specs=placed,
        out_specs=(P("rep", "fsdp", None), P("fsdp", "rep", None, None, None)),
        check_vma=False,
    )
```

```python
import functools
import math

import jax
import jax.numpy as jnp
from jax import lax
from jax.experimental import pallas as pl
from jax.experimental.pallas import tpu as pltpu
from jax.sharding import PartitionSpec as P

NS_ITERS = 5


DECAY = 0.9
DAMPING = 64.0
FIRST_AXES = (((0,), (0,)), ((), ()))
LAST_AXES = (((1,), (1,)), ((), ()))


def inverse_root(matrix, epsilon):
    identity = jnp.eye(matrix.shape[0], dtype=jnp.float32)
    trace_sum = jnp.trace(matrix) + epsilon
    current = matrix / trace_sum
    inverse = identity
    for repeat in range(NS_ITERS):
        middle = 1.5 * identity - 0.5 * jnp.dot(inverse, current, precision=lax.Precision.HIGHEST)
        current = jnp.dot(current, middle, precision=lax.Precision.HIGHEST)
        inverse = jnp.dot(middle, inverse, precision=lax.Precision.HIGHEST)
    return inverse / jnp.sqrt(trace_sum)


def precondition(gradient, current_sketch):
    identity = jnp.eye(current_sketch.shape[1], dtype=jnp.float32)
    projected = lax.dot_general(
        gradient, current_sketch, FIRST_AXES, preferred_element_type=jnp.float32
    ).astype(jnp.bfloat16)
    gram_matrix = lax.dot_general(
        current_sketch, current_sketch, FIRST_AXES, preferred_element_type=jnp.float32
    ).astype(jnp.bfloat16)
    powered = DECAY * jnp.dot(
        current_sketch, gram_matrix, preferred_element_type=jnp.float32
    ) + jnp.dot(gradient, projected, preferred_element_type=jnp.float32)
    inner_gram = lax.dot_general(powered, powered, FIRST_AXES, precision=lax.Precision.HIGHEST)
    basis_full = jnp.dot(powered, inverse_root(inner_gram, 1e-06), precision=lax.Precision.HIGHEST)
    basis_low = basis_full.astype(jnp.bfloat16)
    coefficients = lax.dot_general(
        gradient, basis_low, FIRST_AXES, preferred_element_type=jnp.float32
    ).astype(jnp.bfloat16)
    alignment = lax.dot_general(
        current_sketch, basis_low, FIRST_AXES, preferred_element_type=jnp.float32
    )
    energy = DECAY * lax.dot_general(
        alignment, alignment, FIRST_AXES, precision=lax.Precision.HIGHEST
    ) + lax.dot_general(coefficients, coefficients, FIRST_AXES, preferred_element_type=jnp.float32)
    root_inverse = inverse_root(energy + DAMPING * identity, 0.0)
    inner_part = jnp.dot(energy, root_inverse, precision=lax.Precision.HIGHEST)
    new_block = jnp.dot(basis_full, inner_part, precision=lax.Precision.HIGHEST).astype(
        jnp.bfloat16
    )
    mix_matrix = math.sqrt(DAMPING) * root_inverse - identity
    side_terms = lax.dot_general(
        coefficients.astype(jnp.float32), mix_matrix, LAST_AXES, precision=lax.Precision.HIGHEST
    ).astype(jnp.bfloat16)
    update_block = (
        gradient.astype(jnp.float32)
        + lax.dot_general(basis_low, side_terms, LAST_AXES, preferred_element_type=jnp.float32)
    ).astype(jnp.bfloat16)
    return (update_block, new_block)


def squared_sum(values):
    wide = values.astype(jnp.float32)
    return jnp.sum(wide * wide)


def process_slot(slot_index, arrived, clip_factor, held_sketches, filled):
    block_width = arrived.shape[-1]
    gradient = (clip_factor * arrived.reshape(block_width, block_width).astype(jnp.float32)).astype(
        jnp.bfloat16
    )
    current_sketch = held_sketches[slot_index]
    active = slot_index < filled
    update_block, new_block = precondition(gradient, current_sketch)
    new_block = jnp.where(active, new_block, current_sketch)
    return (update_block, new_block)


def local(partials, sketch, owner_table):
    block_total = partials.shape[1]
    row_count = partials.shape[2]
    block_width = partials.shape[3]
    fsdp_count = lax.axis_size("fsdp")
    per_slice = block_total // lax.axis_size("rep")
    slot_count = sketch.shape[2]
    reduced = lax.psum_scatter(
        partials[0].astype(jnp.float32).astype(jnp.bfloat16), "rep", scatter_dimension=0, tiled=True
    )
    my_owners = lax.dynamic_slice_in_dim(
        owner_table[:, 0], lax.axis_index("rep") * per_slice, per_slice
    )
    positions = jnp.arange(per_slice, dtype=jnp.int32)
    same_owner = (my_owners[:, None] == my_owners[None, :]) & (
        positions[:, None] < positions[None, :]
    )
    rank_in = jnp.sum(same_owner.astype(jnp.int32), axis=0)
    target = rank_in * fsdp_count + my_owners
    selector = (
        target[None, :] == jnp.arange(slot_count * fsdp_count, dtype=jnp.int32)[:, None]
    ).astype(jnp.bfloat16)
    flattened = reduced.reshape(per_slice, row_count * block_width)
    outgoing = jnp.dot(selector, flattened, preferred_element_type=jnp.float32).astype(jnp.bfloat16)
    outgoing = outgoing.reshape(slot_count, fsdp_count, row_count, block_width)
    sum_squares = lax.psum(squared_sum(reduced), ("fsdp", "rep"))
    clip_limit = 0.5 * math.sqrt(block_total * block_width * block_width)
    clip_factor = jnp.minimum(1.0, clip_limit / jnp.sqrt(sum_squares + 1e-06))
    filled = jnp.sum((my_owners == lax.axis_index("fsdp")).astype(jnp.int32))
    held_sketches = sketch[0, 0]
    fresh_list = []
    incoming = lax.all_to_all(outgoing, "fsdp", split_axis=1, concat_axis=1, tiled=True)
    update_list = []
    for slot_index in range(slot_count):
        update_block, new_block = process_slot(
            slot_index, incoming[slot_index], clip_factor, held_sketches, filled
        )
        update_list.append(update_block)
        fresh_list.append(new_block)
    stacked = jnp.stack(update_list).reshape(slot_count, fsdp_count, row_count, block_width)
    returned = lax.all_to_all(stacked, "fsdp", split_axis=1, concat_axis=1, tiled=True)
    returned = returned.reshape(slot_count * fsdp_count, row_count * block_width)
    my_updates = lax.dot_general(
        selector, returned, FIRST_AXES, preferred_element_type=jnp.float32
    ).astype(jnp.bfloat16)
    my_updates = my_updates.reshape(per_slice, row_count, block_width)
    return (my_updates, jnp.stack(fresh_list)[None, None])

MESH = pl.DeviceIdType.MESH
BF = jnp.bfloat16
F32 = jnp.float32


def flip(value, mask, bits):
    result = 0
    for bit in range(bits):
        ours = (value // (1 << bit)) % 2
        theirs = (mask // (1 << bit)) % 2
        result = result + (ours + theirs - 2 * ours * theirs) * (1 << bit)
    return result


def greet(peers):
    barrier = pltpu.get_barrier_semaphore()
    for peer in peers:
        pl.semaphore_signal(barrier, inc=1, device_id=peer, device_id_type=MESH)
    pl.semaphore_wait(barrier, len(peers))


def remote(source, target, send_sem, recv_sem, peer):
    return pltpu.make_async_remote_copy(
        src_ref=source,
        dst_ref=target,
        send_sem=send_sem,
        recv_sem=recv_sem,
        device_id=peer,
        device_id_type=MESH,
    )


def mm(a, b):
    return jnp.dot(a, b, preferred_element_type=F32)


def mm_last(a, b):
    return lax.dot_general(a, b, LAST_AXES, preferred_element_type=F32)


def split(values):
    high = values.astype(BF)
    return high, (values - high.astype(F32)).astype(BF)


def mm3(a, b):
    return mm(a[0], b[0]) + (mm(a[0], b[1]) + mm(a[1], b[0]))


def eye_of(size):
    return (
        lax.broadcasted_iota(jnp.int32, (size, size), 0)
        == lax.broadcasted_iota(jnp.int32, (size, size), 1)
    ).astype(F32)


def kernel_root(matrix, epsilon, identity):
    trace_sum = jnp.sum(matrix * identity, keepdims=True) + epsilon
    current = matrix / trace_sum
    middle = 1.5 * identity - 0.5 * current
    middle_s = split(middle)
    inverse_s = middle_s
    current_s = split(mm3(split(current), middle_s))
    for repeat in range(1, NS_ITERS):
        middle_s = split(1.5 * identity - 0.5 * mm3(inverse_s, current_s))
        if repeat < NS_ITERS - 1:
            current_s = split(mm3(current_s, middle_s))
        inverse = mm3(middle_s, inverse_s)
        inverse_s = split(inverse)
    return inverse / jnp.sqrt(trace_sum)


def cell_order(fsdp, slots, per_slice):
    half = fsdp // 2
    near = range(half - 1, 0, -1)
    cells = [(k, mask) for k in range(slots) for mask in range(fsdp - 1, half - 1, -1)]
    cells += [(0, mask) for mask in near]
    rest = [(k, mask) for k in range(1, slots) for mask in near]
    kept = len(rest) - (slots * fsdp - per_slice)
    return cells + rest[:kept] + [(k, 0) for k in range(slots)] + rest[kept:]


def look_up(index, entries):
    result = 0
    for n, entry in enumerate(entries):
        result = result + jnp.where(index == n, entry, 0)
    return result


def step_kernel(
    fsdp, slots, per_slice, clip_limit, owners_ref, sketch_ref, partials_ref, returned_ref, fresh_ref,
    held_0, held_1, held_2, held_3, sketch_held, staged, paired, crossed, totals, summed, incoming, updates, landing, factor_in, basis_in, narrow_t, side_t, wide, basis, basis_low,
    square_acc, rep_squares, fsdp_squares, half_squares, table, scalars,
    load_sems, pair_sems, cross_sems, owner_sems, rep_sems, fsdp_sems, home_sems, self_sems, table_sem,
    basis_sends, basis_recvs, factor_sends, factor_recvs, land_sends, land_recvs, far_sems, half_sends, half_recv,
):
    bits = fsdp.bit_length() - 1
    half = fsdp // 2
    steps = slots * fsdp
    empty = steps - per_slice
    cells = cell_order(fsdp, slots, per_slice)

    def spot_of(k, mask):
        return look_up(k * fsdp + mask, [cells.index((n // fsdp, n % fsdp)) for n in range(steps)])

    rows = incoming.shape[2]
    width = incoming.shape[3]
    rank = sketch_ref.shape[2]
    tile = rank
    me_f = lax.axis_index("fsdp")
    me_r = lax.axis_index("rep")
    core = me_r % 2
    row = me_r // 2
    partner = row * 2 + 1 - core
    across = (1 - row) * 2 + core
    partner_across = (1 - row) * 2 + 1 - core
    slices = (partner_across, partner, across, me_r)
    held = (held_0, held_1, held_2, held_3)
    loads = [
        pltpu.make_async_copy(
            partials_ref.at[0, pl.ds(number * per_slice, per_slice)], held[n], load_sems.at[n]
        )
        for n, number in enumerate(slices)
    ]
    loads.append(pltpu.make_async_copy(sketch_ref, sketch_held, load_sems.at[len(slices)]))
    for load in loads:
        load.start()
    fill_table(fsdp, slots, per_slice, me_f, owners_ref, table)
    publish = pltpu.make_async_copy(table, scalars, table_sem)
    publish.start()
    greet(
        [{"rep": (me_r + d) % 4} for d in range(1, 4)]
        + [{"fsdp": (me_f + d) % fsdp} for d in range(1, fsdp)]
    )
    square_acc[...] = jnp.zeros_like(square_acc)
    publish.wait()
    loads[0].wait()
    loads[1].wait()

    def block_at(n, k):
        return held[n][scalars[0, slices[n] * per_slice + k]]

    def stage_ref(n, k):
        return updates.at[k // fsdp, k % fsdp] if n == 0 else staged.at[k]

    def pair_copy(n, k):
        return remote(
            stage_ref(n, k), paired.at[n, k], pair_sems.at[0, n, k], pair_sems.at[1, n, k], {"rep": partner}
        )

    def stage(k, carry):
        for n in range(2):
            stage_ref(n, k)[...] = block_at(n, k)
            pair_copy(n, k).start()
        return carry

    lax.fori_loop(0, per_slice, stage, 0)
    for n in range(empty):
        totals[n] = jnp.zeros_like(totals[n])
        totals[empty + per_slice + n] = jnp.zeros_like(totals[n])
    for load in loads[2:]:
        load.wait()

    def where(i):
        code = look_up(i, [k * fsdp + mask for k, mask in cells])
        return code // fsdp, code % fsdp, flip(me_f, code % fsdp, bits)

    def cross_copy(k):
        return remote(
            paired.at[0, k], crossed.at[k], cross_sems.at[0, k], cross_sems.at[1, k], {"rep": across}
        )

    def owner_copy(i):
        slot, mask, owner = where(i)
        return remote(
            summed.at[i],
            incoming.at[slot, me_f],
            owner_sems.at[0, i],
            owner_sems.at[1, i],
            {"fsdp": owner},
        )

    def send_across(k):
        pair_copy(0, k).wait_recv()
        paired[0, k] = (block_at(2, k).astype(F32) + paired[0, k].astype(F32)).astype(BF)
        cross_copy(k).start()

    def add_up(k):
        pair_copy(1, k).wait_recv()
        pair = block_at(3, k).astype(F32) + paired[1, k].astype(F32)
        cross_copy(k).wait_recv()
        total = (pair + crossed[k].astype(F32)).astype(BF)
        totals[empty + k] = total
        wide_total = total.astype(F32)
        square_acc[...] += jnp.sum((wide_total * wide_total).reshape(rows // 8, 8, width), axis=0)

    def send_owner(i):
        slot, mask, owner = where(i)
        skipped = scalars[1, me_r * steps + i]
        total = totals[empty + i]
        for n in range(1, empty + 1):
            total = jnp.where(skipped == n, totals[empty + i - n], total)

        @pl.when(mask == 0)
        def _():
            incoming[slot, me_f] = total

        @pl.when(mask != 0)
        def _():
            summed[i] = total
            owner_copy(i).start()

    lag = 3

    def first(k, carry):
        send_across(k)
        return carry

    lax.fori_loop(0, lag, first, 0)

    def both(k, carry):
        @pl.when(k < per_slice - lag)
        def _():
            send_across(k + lag)

        add_up(k)
        send_owner(k)
        return carry

    lax.fori_loop(0, per_slice, both, 0)

    def arrived(k):
        def wait_one(mask, carry):
            owner_copy(spot_of(k, mask)).wait_recv()
            return carry

        lax.fori_loop(1, fsdp, wait_one, 0)

    def wide_part(k, part):
        return incoming[k, :, :, part * tile : (part + 1) * tile].reshape(width, tile)

    def project(k, left_t, factor):
        for part in range(width // tile):
            product = mm(left_t, wide_part(k, part))
            if factor is not None:
                product = factor * product
            narrow_t[:, part * tile : (part + 1) * tile] = product.astype(BF)

    lanes = square_acc[:, 0:128]
    for part in range(1, width // 128):
        lanes = lanes + square_acc[:, part * 128 : (part + 1) * 128]
    rep_squares[me_r] = lanes
    rep_copies = [
        remote(
            rep_squares.at[me_r], rep_squares.at[me_r], rep_sems.at[0, d], rep_sems.at[1, d],
            {"rep": (me_r + d) % 4},
        )
        for d in range(1, 4)
    ]
    for copy in rep_copies:
        copy.start()
    arrived(0)
    sketch_t = sketch_held[0].T
    project(0, sketch_t, None)
    for copy in rep_copies:
        copy.wait()
    lanes = rep_squares[0]
    for r in range(1, 4):
        lanes = lanes + rep_squares[r]
    fsdp_squares[me_f] = lanes
    half_copies = [
        remote(
            fsdp_squares.at[me_f], fsdp_squares.at[me_f], fsdp_sems.at[0, mask], fsdp_sems.at[1, mask],
            {"fsdp": flip(me_f, mask, bits)},
        )
        for mask in range(1, half)
    ]
    for copy in half_copies:
        copy.start()

    def last(i, carry):
        send_owner(i)
        return carry

    lax.fori_loop(per_slice, steps, last, 0)

    def staged_out(k, carry):
        for n in range(2):
            pair_copy(n, k).wait_send()
        cross_copy(k).wait_send()
        return carry

    lax.fori_loop(0, per_slice, staged_out, 0)
    side = me_f % 2
    top = me_f // half
    base = half * top
    other = half - base
    parts = width // tile
    groups = half // 2
    at_end = me_f // 2 == top * (2 * groups - 1)
    for copy in half_copies:
        copy.wait()
    lanes = fsdp_squares[base]
    for e in range(1, half):
        lanes = lanes + fsdp_squares[base + e]
    half_squares[top] = lanes

    def half_copy(source, e):
        return remote(
            half_squares.at[source], half_squares.at[source], half_sends.at[e], half_recv,
            {"fsdp": other + 2 * e + side},
        )

    @pl.when(at_end)
    def _():
        for e in range(groups):
            half_copy(top, e).start()

    identity = eye_of(rank)
    relay = half + side - 2 * top
    is_relay = me_f // 2 == groups - 1 + top

    def columns(p):
        return pl.ds(pl.multiple_of(p * tile, tile), tile)

    def basis_copy(k, group):
        return remote(
            basis_low.at[k, pl.ds(pl.multiple_of(other * rows, rows), half * rows)],
            basis_in.at[k, group],
            basis_sends.at[k],
            basis_recvs.at[k, group],
            {"fsdp": relay},
        )

    def factor_copy(k, group, p):
        return remote(
            side_t.at[k, :, columns(p)],
            factor_in.at[k, group, :, columns(p)],
            factor_sends.at[k, p],
            factor_recvs.at[k, group, p],
            {"fsdp": relay},
        )

    def land_copy(k, group, e, p):
        return remote(
            incoming.at[k, group * half + e, :, columns(p)],
            landing.at[k, 2 * group + side, :, columns(p)],
            land_sends.at[k, group, e, p],
            land_recvs.at[k, 2 * group + side, p],
            {"fsdp": base + e},
        )

    def landed(k, q, p):
        return remote(
            incoming.at[k, q, :, columns(p)],
            landing.at[k, q, :, columns(p)],
            land_sends.at[k, 0, 0, p],
            land_recvs.at[k, q, p],
            {"fsdp": relay},
        )

    def home_copy(k, mask):
        return remote(
            updates.at[k, mask], returned_ref.at[k, me_f], home_sems.at[0, k, mask], home_sems.at[1, k, mask],
            {"fsdp": flip(me_f, mask, bits)},
        )

    def self_copy(k):
        return pltpu.make_async_copy(updates.at[k, 0], returned_ref.at[k, me_f], self_sems.at[k])

    def far_copy(k, m):
        return pltpu.make_async_copy(
            summed.at[spot_of(k, half + m)],
            returned_ref.at[k, flip(me_f, half + m, bits)],
            far_sems.at[k, m],
        )

    def pass_on(k, turn, begin, end):
        group = turn * top + (groups - 1 - turn) * (1 - top)

        def step(p, carry):
            factor_copy(k, group, p).wait_recv()
            product = mm(basis_in[k, group], factor_in[k, group, :, columns(p)]).astype(BF)
            for e in range(half):
                piece = product[e * rows : (e + 1) * rows]

                @pl.when(e == me_f - base)
                def _():
                    landing[k, 2 * group + side, :, columns(p)] = piece

                @pl.when(e != me_f - base)
                def _():
                    incoming[k, group * half + e, :, columns(p)] = piece
                    land_copy(k, group, e, p).start()

            return carry

        @pl.when(is_relay)
        def _():
            if begin == 0:
                basis_copy(k, group).wait_recv()
            lax.fori_loop(begin, end, step, 0)

    def combine(k):
        def one(m, carry):
            q = flip(me_f, half + m, bits) - other
            i = spot_of(k, half + m)
            owner_copy(i).wait_send()

            @pl.when((q % 2 != side) | (me_f // 2 != groups - 1 + top))
            def _():
                for p in range(parts):
                    landed(k, q, p).wait_recv()

            gradient = (clip_factor * summed[i].astype(F32)).astype(BF).astype(F32)
            summed[i] = (gradient + landing[k, q].astype(F32)).astype(BF)
            far_copy(k, m).start()
            return carry

        lax.fori_loop(0, half, one, 0)

    clip_factor = None
    for k in range(slots):
        sketch = sketch_held[k]
        if k > 0:
            arrived(k)
            sketch_t = sketch.T
            project(k, sketch_t, None)
        gram = mm(sketch_t, sketch).astype(BF)
        projected_t = narrow_t[...]
        for part in range(fsdp):
            span = slice(part * rows, (part + 1) * rows)
            wide[span] = mm_last(incoming[k, part], projected_t)
            basis[span] = DECAY * mm(sketch[span], gram)
        if k == 0:
            half_copy(1 - top, 0).wait_recv()
            lanes = half_squares[0] + half_squares[1]
            sum_squares = jnp.sum(lanes, keepdims=True)
            clip_factor = jnp.minimum(1.0, clip_limit / jnp.sqrt(sum_squares + 1e-06))
        powered_s = split(basis[...] + (clip_factor * clip_factor) * wide[...])
        powered_t = powered_s[0].T
        mixed = mm(powered_t, powered_s[1])
        inner = mm(powered_t, powered_s[0]) + (mixed + mixed.T)
        root = split(kernel_root(inner, 1e-06, identity))
        full = mm3(powered_s, root)
        basis[...] = full
        low = full.astype(BF)
        basis_low[k] = low
        basis_copy(k, me_f % half // 2).start()
        project(k, low.T, clip_factor)
        coefficients_t = narrow_t[...]
        align_s = split(mm(sketch_t, low))
        align_t = (align_s[0].T, align_s[1].T)
        energy = DECAY * mm3(align_t, align_s) + mm_last(coefficients_t, coefficients_t)
        root_inverse = kernel_root(energy + DAMPING * identity, 0.0, identity)
        mix = split(math.sqrt(DAMPING) * root_inverse - identity)
        for part in range(parts):
            span = slice(part * tile, (part + 1) * tile)
            chosen = coefficients_t[:, span]
            side_t[k, :, span] = (mm(mix[0], chosen) + mm(mix[1], chosen)).astype(BF)
            factor_copy(k, me_f % half // 2, part).start()

        def send(i, carry):
            mask = half - 1 - i
            home = flip(me_f, mask, bits)
            start = pl.multiple_of(home * rows, rows)
            gradient = (clip_factor * incoming[k, home].astype(F32)).astype(BF).astype(F32)
            updates[k, mask] = (
                gradient + mm(basis_low[k, pl.ds(start, rows), :], side_t[k])
            ).astype(BF)

            @pl.when(mask == 0)
            def _():
                self_copy(k).start()

            @pl.when(mask != 0)
            def _():
                home_copy(k, mask).start()

            return carry

        lax.fori_loop(0, half, send, 0)
        inner_part = split(mm3(split(energy), split(root_inverse)))
        new_block = mm3(split(basis[...]), inner_part).astype(BF)
        active = scalars[2, me_r * steps + cells.index((k, 0))]
        fresh_ref[k] = jnp.where(active > 0, new_block, sketch)

    split_at = parts // 2
    if slots == 2 and groups == 2:
        pass_on(0, 0, 0, parts)
        pass_on(1, 0, 0, parts)
        pass_on(0, 1, 0, parts)
        pass_on(1, 1, 0, split_at)
        combine(0)
        pass_on(1, 1, split_at, parts)
        combine(1)
    else:
        for k in range(slots):
            for turn in range(groups):
                pass_on(k, turn, 0, parts)
            combine(k)

    def finish(mask, carry):
        for k in range(slots):
            owner_copy(spot_of(k, mask)).wait_send()
            home_copy(k, mask).wait()
        return carry

    lax.fori_loop(1, half, finish, 0)

    @pl.when(at_end)
    def _():
        for e in range(groups):
            half_copy(top, e).wait_send()


    def finish_parts(p, carry):
        for k in range(slots):
            factor_copy(k, 0, p).wait_send()
        return carry

    lax.fori_loop(0, parts, finish_parts, 0)

    @pl.when(is_relay)
    def _():
        def drain(n, carry):
            group = n // (half * parts)
            e = n // parts % half

            @pl.when(e != me_f - base)
            def _():
                for k in range(slots):
                    land_copy(k, group, e, n % parts).wait_send()

            return carry

        lax.fori_loop(0, groups * half * parts, drain, 0)

    def finish_far(m, carry):
        for k in range(slots):
            far_copy(k, m).wait()
        return carry

    lax.fori_loop(0, half, finish_far, 0)
    for k in range(slots):
        basis_copy(k, 0).wait_send()
        self_copy(k).wait()


def fill_table(fsdp, slots, per_slice, me_f, owners_ref, table):
    total = owners_ref.shape[1]
    steps = slots * fsdp
    cells = cell_order(fsdp, slots, per_slice)
    shape = (total, total)
    down = lax.broadcasted_iota(jnp.int32, shape, 0)
    along = lax.broadcasted_iota(jnp.int32, shape, 1)

    def turned(values):
        return jnp.sum(jnp.where(down == along, values, 0), axis=0, keepdims=True)

    owners_along = jnp.broadcast_to(owners_ref[...], shape)
    owners = jnp.sum(jnp.where(down == along, owners_along, 0), axis=1, keepdims=True)
    owners = jnp.broadcast_to(owners, shape)
    same = down // per_slice == along // per_slice
    earlier = same & (owners == owners_along) & (along < down)
    ranks = jnp.sum(jnp.where(earlier, 1, 0), axis=1, keepdims=True)
    mask = lax.bitwise_xor(owners, jnp.full(shape, me_f, jnp.int32))
    cell = jnp.broadcast_to(ranks, shape) * fsdp + mask
    spot = look_up(cell, [cells.index((n // fsdp, n % fsdp)) for n in range(steps)])
    ahead = jnp.sum(jnp.where(same & (turned(spot) < spot), 1, 0), axis=1, keepdims=True)
    spots = jnp.max(spot, axis=1, keepdims=True)
    shape = (total, table.shape[1])
    block = lax.broadcasted_iota(jnp.int32, shape, 0)
    lane = lax.broadcasted_iota(jnp.int32, shape, 1)
    group = block // per_slice
    hit = group * per_slice + jnp.broadcast_to(ahead, shape) == lane
    number = jnp.sum(jnp.where(hit, block % per_slice, 0), axis=0, keepdims=True)
    table[0:1, :] = jnp.minimum(number, per_slice - 1)
    ours = group == lane // steps
    spots = jnp.broadcast_to(spots, shape)
    before = jnp.sum(jnp.where(ours & (spots < lane % steps), 1, 0), axis=0, keepdims=True)
    table[1:2, :] = lane[0:1, :] % steps - before
    table[2:3, :] = jnp.sum(jnp.where(ours & (spots == lane % steps), 1, 0), axis=0, keepdims=True)


def place_kernel(fsdp, per_slice, owners_ref, returned_ref, update_ref, held, counts, in_sems, out_sems):
    base = lax.axis_index("rep") * per_slice
    last = returned_ref.shape[0] - 1
    for owner in range(fsdp):
        counts[owner] = 0
    takes, puts = [], []
    for b in range(per_slice):
        owner = owners_ref[base + b]
        count = counts[owner]
        counts[owner] = count + 1
        takes.append(
            pltpu.make_async_copy(returned_ref.at[jnp.minimum(count, last), owner], held.at[b], in_sems.at[b])
        )
        takes[-1].start()
    for b in range(per_slice):
        takes[b].wait()
        puts.append(pltpu.make_async_copy(held.at[b], update_ref.at[b], out_sems.at[b]))
        puts[-1].start()
    for put in puts:
        put.wait()


def fused(partials, sketch, owner_table):
    block_total, rows, width = partials.shape[1:]
    rank = sketch.shape[4]
    fsdp = lax.axis_size("fsdp")
    rep = lax.axis_size("rep")
    slots = sketch.shape[2]
    per_slice = block_total // rep
    steps = slots * fsdp
    table_width = -(-max(rep * steps, block_total) // 128) * 128
    hbm = pl.BlockSpec(memory_space=pl.ANY)
    vmem = pl.BlockSpec(memory_space=pltpu.VMEM)
    smem = pl.BlockSpec(memory_space=pltpu.SMEM)
    dma = pltpu.SemaphoreType.DMA
    block = (rows, width)
    half = fsdp // 2
    groups = half // 2
    parts = width // rank
    clip_limit = 0.5 * math.sqrt(block_total * width * width)
    returned, fresh = pl.pallas_call(
        functools.partial(step_kernel, fsdp, slots, per_slice, clip_limit),
        out_shape=(
            jax.ShapeDtypeStruct((slots, fsdp) + block, BF),
            jax.ShapeDtypeStruct((slots, width, rank), BF),
        ),
        in_specs=[vmem, hbm, hbm],
        out_specs=(hbm, vmem),
        scratch_shapes=[
            pltpu.VMEM((per_slice,) + block, BF),
            pltpu.VMEM((per_slice,) + block, BF),
            pltpu.VMEM((per_slice,) + block, BF),
            pltpu.VMEM((per_slice,) + block, BF),
            pltpu.VMEM((slots, width, rank), BF),
            pltpu.VMEM((per_slice,) + block, BF),
            pltpu.VMEM((2, per_slice) + block, BF),
            pltpu.VMEM((per_slice,) + block, BF),
            pltpu.VMEM((2 * steps - per_slice,) + block, BF),
            pltpu.VMEM((steps,) + block, BF),
            pltpu.VMEM((slots, fsdp) + block, BF),
            pltpu.VMEM((slots, fsdp) + block, BF),
            pltpu.VMEM((slots, half) + block, BF),
            pltpu.VMEM((slots, groups, rank, width), BF),
            pltpu.VMEM((slots, groups, half * rows, rank), BF),
            pltpu.VMEM((rank, width), BF),
            pltpu.VMEM((slots, rank, width), BF),
            pltpu.VMEM((width, rank), F32),
            pltpu.VMEM((width, rank), F32),
            pltpu.VMEM((slots, width, rank), BF),
            pltpu.VMEM((8, width), F32),
            pltpu.VMEM((rep, 8, 128), F32),
            pltpu.VMEM((fsdp, 8, 128), F32),
            pltpu.VMEM((2, 8, 128), F32),
            pltpu.VMEM((3, table_width), jnp.int32),
            pltpu.SMEM((3, table_width), jnp.int32),
            dma((rep + 1,)),
            dma((2, 2, per_slice)),
            dma((2, per_slice)),
            dma((2, steps)),
            dma((2, rep)),
            dma((2, fsdp)),
            dma((2, slots, half)),
            dma((slots,)),
            dma,
            dma((slots,)),
            dma((slots, groups)),
            dma((slots, parts)),
            dma((slots, groups, parts)),
            dma((slots, groups, half, parts)),
            dma((slots, half, parts)),
            dma((slots, half)),
            dma((groups,)),
            dma,
        ],
        compiler_params=pltpu.CompilerParams(
            collective_id=0, has_side_effects=True, vmem_limit_bytes=VMEM_BYTES
        ),
        name="step",
    )(owner_table.reshape(1, block_total), sketch[0, 0], partials)
    updates = pl.pallas_call(
        functools.partial(place_kernel, fsdp, per_slice),
        out_shape=jax.ShapeDtypeStruct((per_slice,) + block, BF),
        in_specs=[smem, hbm],
        out_specs=hbm,
        scratch_shapes=[
            pltpu.VMEM((per_slice,) + block, BF),
            pltpu.SMEM((fsdp,), jnp.int32),
            dma((per_slice,)),
            dma((per_slice,)),
        ],
        name="place",
    )(owner_table.reshape(block_total), returned)
    return (updates, fresh[None, None])


VMEM_BYTES = 62 * 1024 * 1024


def choose(partials, sketch, owner_table):
    block_total, rows, width = partials.shape[1:]
    fsdp = lax.axis_size("fsdp")
    rep = lax.axis_size("rep")
    steps = sketch.shape[2] * fsdp
    per_slice = block_total // rep
    pairs = rep == 4 and fsdp & (fsdp - 1) == 0 and fsdp >= 4 and steps >= per_slice >= steps - (fsdp // 2 - 1) * (sketch.shape[2] - 1)
    needed = (7 * per_slice + 5 * steps) * rows * width * 2
    if pairs and needed < VMEM_BYTES - (10 << 20):
        return fused(partials, sketch, owner_table)
    return local(partials, sketch, owner_table)


def solution(mesh):
    placed = (P("rep", None, "fsdp", None), P("fsdp", "rep", None, None, None), P())
    return jax.shard_map(
        choose,
        mesh=mesh,
        in_specs=placed,
        out_specs=(P("rep", "fsdp", None), P("fsdp", "rep", None, None, None)),
        check_vma=False,
    )
```

```python
import functools
import math

import jax
import jax.numpy as jnp
from jax import lax
from jax.experimental import pallas as pl
from jax.experimental.pallas import tpu as pltpu
from jax.sharding import PartitionSpec as P

NS_ITERS = 5


DECAY = 0.9
DAMPING = 64.0
FIRST_AXES = (((0,), (0,)), ((), ()))
LAST_AXES = (((1,), (1,)), ((), ()))


def inverse_root(matrix, epsilon):
    identity = jnp.eye(matrix.shape[0], dtype=jnp.float32)
    trace_sum = jnp.trace(matrix) + epsilon
    current = matrix / trace_sum
    inverse = identity
    for repeat in range(NS_ITERS):
        middle = 1.5 * identity - 0.5 * jnp.dot(inverse, current, precision=lax.Precision.HIGHEST)
        current = jnp.dot(current, middle, precision=lax.Precision.HIGHEST)
        inverse = jnp.dot(middle, inverse, precision=lax.Precision.HIGHEST)
    return inverse / jnp.sqrt(trace_sum)


def precondition(gradient, current_sketch):
    identity = jnp.eye(current_sketch.shape[1], dtype=jnp.float32)
    projected = lax.dot_general(
        gradient, current_sketch, FIRST_AXES, preferred_element_type=jnp.float32
    ).astype(jnp.bfloat16)
    gram_matrix = lax.dot_general(
        current_sketch, current_sketch, FIRST_AXES, preferred_element_type=jnp.float32
    ).astype(jnp.bfloat16)
    powered = DECAY * jnp.dot(
        current_sketch, gram_matrix, preferred_element_type=jnp.float32
    ) + jnp.dot(gradient, projected, preferred_element_type=jnp.float32)
    inner_gram = lax.dot_general(powered, powered, FIRST_AXES, precision=lax.Precision.HIGHEST)
    basis_full = jnp.dot(powered, inverse_root(inner_gram, 1e-06), precision=lax.Precision.HIGHEST)
    basis_low = basis_full.astype(jnp.bfloat16)
    coefficients = lax.dot_general(
        gradient, basis_low, FIRST_AXES, preferred_element_type=jnp.float32
    ).astype(jnp.bfloat16)
    alignment = lax.dot_general(
        current_sketch, basis_low, FIRST_AXES, preferred_element_type=jnp.float32
    )
    energy = DECAY * lax.dot_general(
        alignment, alignment, FIRST_AXES, precision=lax.Precision.HIGHEST
    ) + lax.dot_general(coefficients, coefficients, FIRST_AXES, preferred_element_type=jnp.float32)
    root_inverse = inverse_root(energy + DAMPING * identity, 0.0)
    inner_part = jnp.dot(energy, root_inverse, precision=lax.Precision.HIGHEST)
    new_block = jnp.dot(basis_full, inner_part, precision=lax.Precision.HIGHEST).astype(
        jnp.bfloat16
    )
    mix_matrix = math.sqrt(DAMPING) * root_inverse - identity
    side_terms = lax.dot_general(
        coefficients.astype(jnp.float32), mix_matrix, LAST_AXES, precision=lax.Precision.HIGHEST
    ).astype(jnp.bfloat16)
    update_block = (
        gradient.astype(jnp.float32)
        + lax.dot_general(basis_low, side_terms, LAST_AXES, preferred_element_type=jnp.float32)
    ).astype(jnp.bfloat16)
    return (update_block, new_block)


def squared_sum(values):
    wide = values.astype(jnp.float32)
    return jnp.sum(wide * wide)


def process_slot(slot_index, arrived, clip_factor, held_sketches, filled):
    block_width = arrived.shape[-1]
    gradient = (clip_factor * arrived.reshape(block_width, block_width).astype(jnp.float32)).astype(
        jnp.bfloat16
    )
    current_sketch = held_sketches[slot_index]
    active = slot_index < filled
    update_block, new_block = precondition(gradient, current_sketch)
    new_block = jnp.where(active, new_block, current_sketch)
    return (update_block, new_block)


def local(partials, sketch, owner_table):
    block_total = partials.shape[1]
    row_count = partials.shape[2]
    block_width = partials.shape[3]
    fsdp_count = lax.axis_size("fsdp")
    per_slice = block_total // lax.axis_size("rep")
    slot_count = sketch.shape[2]
    reduced = lax.psum_scatter(
        partials[0].astype(jnp.float32).astype(jnp.bfloat16), "rep", scatter_dimension=0, tiled=True
    )
    my_owners = lax.dynamic_slice_in_dim(
        owner_table[:, 0], lax.axis_index("rep") * per_slice, per_slice
    )
    positions = jnp.arange(per_slice, dtype=jnp.int32)
    same_owner = (my_owners[:, None] == my_owners[None, :]) & (
        positions[:, None] < positions[None, :]
    )
    rank_in = jnp.sum(same_owner.astype(jnp.int32), axis=0)
    target = rank_in * fsdp_count + my_owners
    selector = (
        target[None, :] == jnp.arange(slot_count * fsdp_count, dtype=jnp.int32)[:, None]
    ).astype(jnp.bfloat16)
    flattened = reduced.reshape(per_slice, row_count * block_width)
    outgoing = jnp.dot(selector, flattened, preferred_element_type=jnp.float32).astype(jnp.bfloat16)
    outgoing = outgoing.reshape(slot_count, fsdp_count, row_count, block_width)
    sum_squares = lax.psum(squared_sum(reduced), ("fsdp", "rep"))
    clip_limit = 0.5 * math.sqrt(block_total * block_width * block_width)
    clip_factor = jnp.minimum(1.0, clip_limit / jnp.sqrt(sum_squares + 1e-06))
    filled = jnp.sum((my_owners == lax.axis_index("fsdp")).astype(jnp.int32))
    held_sketches = sketch[0, 0]
    fresh_list = []
    incoming = lax.all_to_all(outgoing, "fsdp", split_axis=1, concat_axis=1, tiled=True)
    update_list = []
    for slot_index in range(slot_count):
        update_block, new_block = process_slot(
            slot_index, incoming[slot_index], clip_factor, held_sketches, filled
        )
        update_list.append(update_block)
        fresh_list.append(new_block)
    stacked = jnp.stack(update_list).reshape(slot_count, fsdp_count, row_count, block_width)
    returned = lax.all_to_all(stacked, "fsdp", split_axis=1, concat_axis=1, tiled=True)
    returned = returned.reshape(slot_count * fsdp_count, row_count * block_width)
    my_updates = lax.dot_general(
        selector, returned, FIRST_AXES, preferred_element_type=jnp.float32
    ).astype(jnp.bfloat16)
    my_updates = my_updates.reshape(per_slice, row_count, block_width)
    return (my_updates, jnp.stack(fresh_list)[None, None])

MESH = pl.DeviceIdType.MESH
BF = jnp.bfloat16
F32 = jnp.float32


def flip(value, mask, bits):
    result = 0
    for bit in range(bits):
        ours = (value // (1 << bit)) % 2
        theirs = (mask // (1 << bit)) % 2
        result = result + (ours + theirs - 2 * ours * theirs) * (1 << bit)
    return result


def greet(peers):
    barrier = pltpu.get_barrier_semaphore()
    for peer in peers:
        pl.semaphore_signal(barrier, inc=1, device_id=peer, device_id_type=MESH)
    pl.semaphore_wait(barrier, len(peers))


def remote(source, target, send_sem, recv_sem, peer):
    return pltpu.make_async_remote_copy(
        src_ref=source,
        dst_ref=target,
        send_sem=send_sem,
        recv_sem=recv_sem,
        device_id=peer,
        device_id_type=MESH,
    )


def mm(a, b):
    return jnp.dot(a, b, preferred_element_type=F32)


def mm_last(a, b):
    return lax.dot_general(a, b, LAST_AXES, preferred_element_type=F32)


def split(values):
    high = values.astype(BF)
    return high, (values - high.astype(F32)).astype(BF)


def mm3(a, b):
    return mm(a[0], b[0]) + (mm(a[0], b[1]) + mm(a[1], b[0]))


def eye_of(size):
    return (
        lax.broadcasted_iota(jnp.int32, (size, size), 0)
        == lax.broadcasted_iota(jnp.int32, (size, size), 1)
    ).astype(F32)


def kernel_root(matrix, epsilon, identity):
    trace_sum = jnp.sum(matrix * identity, keepdims=True) + epsilon
    current = matrix / trace_sum
    middle = 1.5 * identity - 0.5 * current
    middle_s = split(middle)
    inverse_s = middle_s
    current_s = split(mm3(split(current), middle_s))
    for repeat in range(1, NS_ITERS):
        middle_s = split(1.5 * identity - 0.5 * mm3(inverse_s, current_s))
        if repeat < NS_ITERS - 1:
            current_s = split(mm3(current_s, middle_s))
        inverse = mm3(middle_s, inverse_s)
        inverse_s = split(inverse)
    return inverse / jnp.sqrt(trace_sum)


def cell_order(fsdp, slots, per_slice):
    half = fsdp // 2
    near = range(half - 1, 0, -1)
    cells = [(k, mask) for k in range(slots) for mask in range(fsdp - 1, half - 1, -1)]
    cells += [(0, mask) for mask in near]
    rest = [(k, mask) for k in range(1, slots) for mask in near]
    kept = len(rest) - (slots * fsdp - per_slice)
    return cells + rest[:kept] + [(k, 0) for k in range(slots)] + rest[kept:]


def look_up(index, entries):
    result = 0
    for n, entry in enumerate(entries):
        result = result + jnp.where(index == n, entry, 0)
    return result


def step_kernel(
    fsdp, slots, per_slice, clip_limit, owners_ref, sketch_ref, partials_ref, returned_ref, fresh_ref,
    held_0, held_1, held_2, held_3, sketch_held, fresh_held, staged, paired, crossed, totals, summed, incoming, updates, landing, factor_in, basis_in, narrow_t, side_t, wide, basis, basis_low,
    square_acc, rep_squares, fsdp_squares, half_squares, table, scalars,
    load_sems, pair_sems, cross_sems, owner_sems, rep_sems, fsdp_sems, home_sems, self_sems, table_sem,
    basis_sends, basis_recvs, factor_sends, factor_recvs, land_sends, land_recvs, far_sems, half_sends, half_recv, fresh_sems,
):
    bits = fsdp.bit_length() - 1
    half = fsdp // 2
    steps = slots * fsdp
    empty = steps - per_slice
    cells = cell_order(fsdp, slots, per_slice)

    def spot_of(k, mask):
        return look_up(k * fsdp + mask, [cells.index((n // fsdp, n % fsdp)) for n in range(steps)])

    rows = incoming.shape[2]
    width = incoming.shape[3]
    rank = sketch_ref.shape[2]
    tile = rank
    me_f = lax.axis_index("fsdp")
    me_r = lax.axis_index("rep")
    core = me_r % 2
    row = me_r // 2
    partner = row * 2 + 1 - core
    across = (1 - row) * 2 + core
    partner_across = (1 - row) * 2 + 1 - core
    slices = (partner_across, partner, across, me_r)
    early = (0, 2)
    held = (held_0, held_1, held_2, held_3)
    loads = [
        pltpu.make_async_copy(
            partials_ref.at[0, pl.ds(number * per_slice, per_slice)], held[n], load_sems.at[n]
        )
        for n, number in enumerate(slices)
    ]
    loads.append(pltpu.make_async_copy(sketch_ref, sketch_held, load_sems.at[len(slices)]))
    for n in early:
        loads[n].start()
    fill_table(fsdp, slots, per_slice, me_f, owners_ref, table)
    publish = pltpu.make_async_copy(table, scalars, table_sem)
    publish.start()
    greet(
        [{"rep": (me_r + d) % 4} for d in range(1, 4)]
        + [{"fsdp": (me_f + d) % fsdp} for d in range(1, fsdp)]
    )
    for n, load in enumerate(loads):
        if n not in early:
            load.start()
    square_acc[...] = jnp.zeros_like(square_acc)
    publish.wait()
    loads[0].wait()

    def block_at(n, k):
        return held[n][scalars[0, slices[n] * per_slice + k]]

    def stage_ref(n, k):
        return updates.at[k // fsdp, k % fsdp] if n == 0 else staged.at[k]

    def pair_copy(n, k):
        return remote(
            stage_ref(n, k), paired.at[n, k], pair_sems.at[0, n, k], pair_sems.at[1, n, k], {"rep": partner}
        )

    def stage(n):
        def step(k, carry):
            stage_ref(n, k)[...] = block_at(n, k)
            pair_copy(n, k).start()
            return carry

        lax.fori_loop(0, per_slice, step, 0)

    stage(0)
    loads[2].wait()

    def where(i):
        code = look_up(i, [k * fsdp + mask for k, mask in cells])
        return code // fsdp, code % fsdp, flip(me_f, code % fsdp, bits)

    def cross_copy(k):
        return remote(
            paired.at[0, k], crossed.at[k], cross_sems.at[0, k], cross_sems.at[1, k], {"rep": across}
        )

    def owner_copy(i):
        slot, mask, owner = where(i)
        return remote(
            summed.at[i],
            incoming.at[slot, me_f],
            owner_sems.at[0, i],
            owner_sems.at[1, i],
            {"fsdp": owner},
        )

    def send_across(k):
        pair_copy(0, k).wait_recv()
        paired[0, k] = (block_at(2, k).astype(F32) + paired[0, k].astype(F32)).astype(BF)
        cross_copy(k).start()

    def add_up(k):
        pair_copy(1, k).wait_recv()
        pair = block_at(3, k).astype(F32) + paired[1, k].astype(F32)
        cross_copy(k).wait_recv()
        total = (pair + crossed[k].astype(F32)).astype(BF)
        totals[empty + k] = total
        wide_total = total.astype(F32)
        square_acc[...] += jnp.sum((wide_total * wide_total).reshape(rows // 8, 8, width), axis=0)

    def send_owner(i):
        slot, mask, owner = where(i)
        skipped = scalars[1, me_r * steps + i]
        total = totals[empty + i]
        for n in range(1, empty + 1):
            total = jnp.where(skipped == n, totals[empty + i - n], total)

        @pl.when(mask == 0)
        def _():
            incoming[slot, me_f] = total

        @pl.when(mask != 0)
        def _():
            summed[i] = total
            owner_copy(i).start()

    lag = 3

    def first(k, carry):
        send_across(k)
        return carry

    lax.fori_loop(0, lag, first, 0)
    loads[1].wait()
    stage(1)
    for n in range(empty):
        totals[n] = jnp.zeros_like(totals[n])
        totals[empty + per_slice + n] = jnp.zeros_like(totals[n])
    for load in loads[3:]:
        load.wait()

    def both(k, carry):
        @pl.when(k < per_slice - lag)
        def _():
            send_across(k + lag)

        add_up(k)
        send_owner(k)
        return carry

    lax.fori_loop(0, per_slice, both, 0)

    def arrived(k):
        def wait_one(mask, carry):
            owner_copy(spot_of(k, mask)).wait_recv()
            return carry

        lax.fori_loop(1, fsdp, wait_one, 0)

    def wide_part(k, part):
        return incoming[k, :, :, part * tile : (part + 1) * tile].reshape(width, tile)

    def project(k, left_t, factor):
        for part in range(width // tile):
            product = mm(left_t, wide_part(k, part))
            if factor is not None:
                product = factor * product
            narrow_t[:, part * tile : (part + 1) * tile] = product.astype(BF)

    lanes = square_acc[:, 0:128]
    for part in range(1, width // 128):
        lanes = lanes + square_acc[:, part * 128 : (part + 1) * 128]
    rep_squares[me_r] = lanes
    rep_copies = [
        remote(
            rep_squares.at[me_r], rep_squares.at[me_r], rep_sems.at[0, d], rep_sems.at[1, d],
            {"rep": (me_r + d) % 4},
        )
        for d in range(1, 4)
    ]
    for copy in rep_copies:
        copy.start()
    arrived(0)
    sketch_t = sketch_held[0].T
    project(0, sketch_t, None)
    for copy in rep_copies:
        copy.wait()
    lanes = rep_squares[0]
    for r in range(1, 4):
        lanes = lanes + rep_squares[r]
    fsdp_squares[me_f] = lanes
    half_copies = [
        remote(
            fsdp_squares.at[me_f], fsdp_squares.at[me_f], fsdp_sems.at[0, mask], fsdp_sems.at[1, mask],
            {"fsdp": flip(me_f, mask, bits)},
        )
        for mask in range(1, half)
    ]
    for copy in half_copies:
        copy.start()

    def last(i, carry):
        send_owner(i)
        return carry

    lax.fori_loop(per_slice, steps, last, 0)

    def staged_out(k, carry):
        for n in range(2):
            pair_copy(n, k).wait_send()
        cross_copy(k).wait_send()
        return carry

    lax.fori_loop(0, per_slice, staged_out, 0)
    side = me_f % 2
    top = me_f // half
    base = half * top
    other = half - base
    parts = width // tile
    groups = half // 2
    at_end = me_f // 2 == top * (2 * groups - 1)
    for copy in half_copies:
        copy.wait()
    lanes = fsdp_squares[base]
    for e in range(1, half):
        lanes = lanes + fsdp_squares[base + e]
    half_squares[top] = lanes

    def half_copy(source, e):
        return remote(
            half_squares.at[source], half_squares.at[source], half_sends.at[e], half_recv,
            {"fsdp": other + 2 * e + side},
        )

    @pl.when(at_end)
    def _():
        for e in range(groups):
            half_copy(top, e).start()

    identity = eye_of(rank)
    relay = half + side - 2 * top
    is_relay = me_f // 2 == groups - 1 + top

    def columns(p):
        return pl.ds(pl.multiple_of(p * tile, tile), tile)

    def basis_copy(k, group):
        return remote(
            basis_low.at[k, pl.ds(pl.multiple_of(other * rows, rows), half * rows)],
            basis_in.at[k, group],
            basis_sends.at[k],
            basis_recvs.at[k, group],
            {"fsdp": relay},
        )

    def factor_copy(k, group, p):
        return remote(
            side_t.at[k, :, columns(p)],
            factor_in.at[k, group, :, columns(p)],
            factor_sends.at[k, p],
            factor_recvs.at[k, group, p],
            {"fsdp": relay},
        )

    def land_copy(k, group, e, p):
        return remote(
            incoming.at[k, group * half + e, :, columns(p)],
            landing.at[k, 2 * group + side, :, columns(p)],
            land_sends.at[k, group, e, p],
            land_recvs.at[k, 2 * group + side, p],
            {"fsdp": base + e},
        )

    def landed(k, q, p):
        return remote(
            incoming.at[k, q, :, columns(p)],
            landing.at[k, q, :, columns(p)],
            land_sends.at[k, 0, 0, p],
            land_recvs.at[k, q, p],
            {"fsdp": relay},
        )

    def home_copy(k, mask):
        return remote(
            updates.at[k, mask], returned_ref.at[k, me_f], home_sems.at[0, k, mask], home_sems.at[1, k, mask],
            {"fsdp": flip(me_f, mask, bits)},
        )

    def fresh_copy(k):
        return pltpu.make_async_copy(fresh_held.at[k], fresh_ref.at[k], fresh_sems.at[k])

    def self_copy(k):
        return pltpu.make_async_copy(updates.at[k, 0], returned_ref.at[k, me_f], self_sems.at[k])

    def far_copy(k, m):
        return pltpu.make_async_copy(
            summed.at[spot_of(k, half + m)],
            returned_ref.at[k, flip(me_f, half + m, bits)],
            far_sems.at[k, m],
        )

    def pass_on(k, turn, begin, end):
        group = turn * top + (groups - 1 - turn) * (1 - top)

        def step(p, carry):
            factor_copy(k, group, p).wait_recv()
            product = mm(basis_in[k, group], factor_in[k, group, :, columns(p)]).astype(BF)
            for e in range(half):
                piece = product[e * rows : (e + 1) * rows]

                @pl.when(e == me_f - base)
                def _():
                    landing[k, 2 * group + side, :, columns(p)] = piece

                @pl.when(e != me_f - base)
                def _():
                    incoming[k, group * half + e, :, columns(p)] = piece
                    land_copy(k, group, e, p).start()

            return carry

        @pl.when(is_relay)
        def _():
            if begin == 0:
                basis_copy(k, group).wait_recv()
            lax.fori_loop(begin, end, step, 0)

    def combine(k):
        def one(m, carry):
            q = flip(me_f, half + m, bits) - other
            i = spot_of(k, half + m)
            owner_copy(i).wait_send()

            @pl.when((q % 2 != side) | (me_f // 2 != groups - 1 + top))
            def _():
                for p in range(parts):
                    landed(k, q, p).wait_recv()

            gradient = (clip_factor * summed[i].astype(F32)).astype(BF).astype(F32)
            summed[i] = (gradient + landing[k, q].astype(F32)).astype(BF)
            far_copy(k, m).start()
            return carry

        lax.fori_loop(0, half, one, 0)

    clip_factor = None
    split_at = parts // 2
    paired_turns = slots == 2 and groups == 2
    for k in range(slots):
        sketch = sketch_held[k]
        if k > 0:
            arrived(k)
            sketch_t = sketch.T
            project(k, sketch_t, None)
        gram = mm(sketch_t, sketch).astype(BF)
        projected_t = narrow_t[...]
        for part in range(fsdp):
            span = slice(part * rows, (part + 1) * rows)
            wide[span] = mm_last(incoming[k, part], projected_t)
            basis[span] = DECAY * mm(sketch[span], gram)
        if k == 0:
            half_copy(1 - top, 0).wait_recv()
            lanes = half_squares[0] + half_squares[1]
            sum_squares = jnp.sum(lanes, keepdims=True)
            clip_factor = jnp.minimum(1.0, clip_limit / jnp.sqrt(sum_squares + 1e-06))
        powered_s = split(basis[...] + (clip_factor * clip_factor) * wide[...])
        powered_t = powered_s[0].T
        mixed = mm(powered_t, powered_s[1])
        inner = mm(powered_t, powered_s[0]) + (mixed + mixed.T)
        root = split(kernel_root(inner, 1e-06, identity))
        full = mm3(powered_s, root)
        basis[...] = full
        low = full.astype(BF)
        basis_low[k] = low
        basis_copy(k, me_f % half // 2).start()
        project(k, low.T, clip_factor)
        if k == 1 and paired_turns:
            pass_on(0, 0, 0, split_at)
        coefficients_t = narrow_t[...]
        align_s = split(mm(sketch_t, low))
        align_t = (align_s[0].T, align_s[1].T)
        energy = DECAY * mm3(align_t, align_s) + mm_last(coefficients_t, coefficients_t)
        root_inverse = kernel_root(energy + DAMPING * identity, 0.0, identity)
        mix = split(math.sqrt(DAMPING) * root_inverse - identity)
        for part in range(parts):
            span = slice(part * tile, (part + 1) * tile)
            chosen = coefficients_t[:, span]
            side_t[k, :, span] = (mm(mix[0], chosen) + mm(mix[1], chosen)).astype(BF)
            factor_copy(k, me_f % half // 2, part).start()

        def send(i, carry):
            mask = half - 1 - i
            home = flip(me_f, mask, bits)
            start = pl.multiple_of(home * rows, rows)
            gradient = (clip_factor * incoming[k, home].astype(F32)).astype(BF).astype(F32)
            updates[k, mask] = (
                gradient + mm(basis_low[k, pl.ds(start, rows), :], side_t[k])
            ).astype(BF)

            @pl.when(mask == 0)
            def _():
                self_copy(k).start()

            @pl.when(mask != 0)
            def _():
                home_copy(k, mask).start()

            return carry

        lax.fori_loop(0, half, send, 0)
        inner_part = split(mm3(split(energy), split(root_inverse)))
        new_block = mm3(split(basis[...]), inner_part).astype(BF)
        active = scalars[2, me_r * steps + cells.index((k, 0))]
        fresh_held[k] = jnp.where(active > 0, new_block, sketch)
        fresh_copy(k).start()

    if paired_turns:
        pass_on(0, 0, split_at, parts)
        pass_on(1, 0, 0, parts)
        pass_on(0, 1, 0, parts)
        pass_on(1, 1, 0, split_at)
        combine(0)
        pass_on(1, 1, split_at, parts)
        combine(1)
    else:
        for k in range(slots):
            for turn in range(groups):
                pass_on(k, turn, 0, parts)
            combine(k)

    def finish(mask, carry):
        for k in range(slots):
            owner_copy(spot_of(k, mask)).wait_send()
            home_copy(k, mask).wait()
        return carry

    lax.fori_loop(1, half, finish, 0)

    @pl.when(at_end)
    def _():
        for e in range(groups):
            half_copy(top, e).wait_send()


    def finish_parts(p, carry):
        for k in range(slots):
            factor_copy(k, 0, p).wait_send()
        return carry

    lax.fori_loop(0, parts, finish_parts, 0)

    @pl.when(is_relay)
    def _():
        def drain(n, carry):
            group = n // (half * parts)
            e = n // parts % half

            @pl.when(e != me_f - base)
            def _():
                for k in range(slots):
                    land_copy(k, group, e, n % parts).wait_send()

            return carry

        lax.fori_loop(0, groups * half * parts, drain, 0)

    def finish_far(m, carry):
        for k in range(slots):
            far_copy(k, m).wait()
        return carry

    lax.fori_loop(0, half, finish_far, 0)
    for k in range(slots):
        basis_copy(k, 0).wait_send()
        self_copy(k).wait()
        fresh_copy(k).wait()


def fill_table(fsdp, slots, per_slice, me_f, owners_ref, table):
    total = owners_ref.shape[1]
    steps = slots * fsdp
    cells = cell_order(fsdp, slots, per_slice)
    shape = (total, total)
    down = lax.broadcasted_iota(jnp.int32, shape, 0)
    along = lax.broadcasted_iota(jnp.int32, shape, 1)

    def turned(values):
        return jnp.sum(jnp.where(down == along, values, 0), axis=0, keepdims=True)

    owners_along = jnp.broadcast_to(owners_ref[...], shape)
    owners = jnp.sum(jnp.where(down == along, owners_along, 0), axis=1, keepdims=True)
    owners = jnp.broadcast_to(owners, shape)
    same = down // per_slice == along // per_slice
    earlier = same & (owners == owners_along) & (along < down)
    ranks = jnp.sum(jnp.where(earlier, 1, 0), axis=1, keepdims=True)
    mask = lax.bitwise_xor(owners, jnp.full(shape, me_f, jnp.int32))
    cell = jnp.broadcast_to(ranks, shape) * fsdp + mask
    spot = look_up(cell, [cells.index((n // fsdp, n % fsdp)) for n in range(steps)])
    ahead = jnp.sum(jnp.where(same & (turned(spot) < spot), 1, 0), axis=1, keepdims=True)
    spots = jnp.max(spot, axis=1, keepdims=True)
    shape = (total, table.shape[1])
    block = lax.broadcasted_iota(jnp.int32, shape, 0)
    lane = lax.broadcasted_iota(jnp.int32, shape, 1)
    group = block // per_slice
    hit = group * per_slice + jnp.broadcast_to(ahead, shape) == lane
    number = jnp.sum(jnp.where(hit, block % per_slice, 0), axis=0, keepdims=True)
    table[0:1, :] = jnp.minimum(number, per_slice - 1)
    ours = group == lane // steps
    spots = jnp.broadcast_to(spots, shape)
    before = jnp.sum(jnp.where(ours & (spots < lane % steps), 1, 0), axis=0, keepdims=True)
    table[1:2, :] = lane[0:1, :] % steps - before
    table[2:3, :] = jnp.sum(jnp.where(ours & (spots == lane % steps), 1, 0), axis=0, keepdims=True)


def place_kernel(
    fsdp, per_slice, owners_ref, returned_ref, fresh_ref, update_ref, kept_ref,
    held, kept, counts, in_sems, out_sems, kept_sems,
):
    base = lax.axis_index("rep") * per_slice
    last = returned_ref.shape[0] - 1
    for owner in range(fsdp):
        counts[owner] = 0
    takes, puts = [], []
    for b in range(per_slice):
        owner = owners_ref[base + b]
        count = counts[owner]
        counts[owner] = count + 1
        takes.append(
            pltpu.make_async_copy(returned_ref.at[jnp.minimum(count, last), owner], held.at[b], in_sems.at[b])
        )
        takes[-1].start()
    take_kept = pltpu.make_async_copy(fresh_ref, kept, kept_sems.at[0])
    take_kept.start()
    for b in range(per_slice):
        takes[b].wait()
        puts.append(pltpu.make_async_copy(held.at[b], update_ref.at[b], out_sems.at[b]))
        puts[-1].start()
    take_kept.wait()
    puts.append(pltpu.make_async_copy(kept, kept_ref, kept_sems.at[1]))
    puts[-1].start()
    for put in puts:
        put.wait()


def fused(partials, sketch, owner_table):
    block_total, rows, width = partials.shape[1:]
    rank = sketch.shape[4]
    fsdp = lax.axis_size("fsdp")
    rep = lax.axis_size("rep")
    slots = sketch.shape[2]
    per_slice = block_total // rep
    steps = slots * fsdp
    table_width = -(-max(rep * steps, block_total) // 128) * 128
    hbm = pl.BlockSpec(memory_space=pl.ANY)
    vmem = pl.BlockSpec(memory_space=pltpu.VMEM)
    smem = pl.BlockSpec(memory_space=pltpu.SMEM)
    dma = pltpu.SemaphoreType.DMA
    block = (rows, width)
    half = fsdp // 2
    groups = half // 2
    parts = width // rank
    clip_limit = 0.5 * math.sqrt(block_total * width * width)
    returned, fresh = pl.pallas_call(
        functools.partial(step_kernel, fsdp, slots, per_slice, clip_limit),
        out_shape=(
            jax.ShapeDtypeStruct((slots, fsdp) + block, BF),
            jax.ShapeDtypeStruct((slots, width, rank), BF),
        ),
        in_specs=[vmem, hbm, hbm],
        out_specs=(hbm, hbm),
        scratch_shapes=[
            pltpu.VMEM((per_slice,) + block, BF),
            pltpu.VMEM((per_slice,) + block, BF),
            pltpu.VMEM((per_slice,) + block, BF),
            pltpu.VMEM((per_slice,) + block, BF),
            pltpu.VMEM((slots, width, rank), BF),
            pltpu.VMEM((slots, width, rank), BF),
            pltpu.VMEM((per_slice,) + block, BF),
            pltpu.VMEM((2, per_slice) + block, BF),
            pltpu.VMEM((per_slice,) + block, BF),
            pltpu.VMEM((2 * steps - per_slice,) + block, BF),
            pltpu.VMEM((steps,) + block, BF),
            pltpu.VMEM((slots, fsdp) + block, BF),
            pltpu.VMEM((slots, fsdp) + block, BF),
            pltpu.VMEM((slots, half) + block, BF),
            pltpu.VMEM((slots, groups, rank, width), BF),
            pltpu.VMEM((slots, groups, half * rows, rank), BF),
            pltpu.VMEM((rank, width), BF),
            pltpu.VMEM((slots, rank, width), BF),
            pltpu.VMEM((width, rank), F32),
            pltpu.VMEM((width, rank), F32),
            pltpu.VMEM((slots, width, rank), BF),
            pltpu.VMEM((8, width), F32),
            pltpu.VMEM((rep, 8, 128), F32),
            pltpu.VMEM((fsdp, 8, 128), F32),
            pltpu.VMEM((2, 8, 128), F32),
            pltpu.VMEM((3, table_width), jnp.int32),
            pltpu.SMEM((3, table_width), jnp.int32),
            dma((rep + 1,)),
            dma((2, 2, per_slice)),
            dma((2, per_slice)),
            dma((2, steps)),
            dma((2, rep)),
            dma((2, fsdp)),
            dma((2, slots, half)),
            dma((slots,)),
            dma,
            dma((slots,)),
            dma((slots, groups)),
            dma((slots, parts)),
            dma((slots, groups, parts)),
            dma((slots, groups, half, parts)),
            dma((slots, half, parts)),
            dma((slots, half)),
            dma((groups,)),
            dma,
            dma((slots,)),
        ],
        compiler_params=pltpu.CompilerParams(
            collective_id=0, has_side_effects=True, vmem_limit_bytes=VMEM_BYTES
        ),
        name="step",
    )(owner_table.reshape(1, block_total), sketch[0, 0], partials)
    updates, kept = pl.pallas_call(
        functools.partial(place_kernel, fsdp, per_slice),
        out_shape=(
            jax.ShapeDtypeStruct((per_slice,) + block, BF),
            jax.ShapeDtypeStruct((slots, width, rank), BF),
        ),
        in_specs=[smem, hbm, hbm],
        out_specs=(hbm, hbm),
        scratch_shapes=[
            pltpu.VMEM((per_slice,) + block, BF),
            pltpu.VMEM((slots, width, rank), BF),
            pltpu.SMEM((fsdp,), jnp.int32),
            dma((per_slice,)),
            dma((per_slice,)),
            dma((2,)),
        ],
        name="place",
    )(owner_table.reshape(block_total), returned, fresh)
    return (updates, kept[None, None])


VMEM_BYTES = 62 * 1024 * 1024


def choose(partials, sketch, owner_table):
    block_total, rows, width = partials.shape[1:]
    fsdp = lax.axis_size("fsdp")
    rep = lax.axis_size("rep")
    steps = sketch.shape[2] * fsdp
    per_slice = block_total // rep
    pairs = rep == 4 and fsdp & (fsdp - 1) == 0 and fsdp >= 4 and steps >= per_slice >= steps - (fsdp // 2 - 1) * (sketch.shape[2] - 1)
    needed = (7 * per_slice + 5 * steps) * rows * width * 2
    if pairs and needed < VMEM_BYTES - (10 << 20):
        return fused(partials, sketch, owner_table)
    return local(partials, sketch, owner_table)


def solution(mesh):
    placed = (P("rep", None, "fsdp", None), P("fsdp", "rep", None, None, None), P())
    return jax.shard_map(
        choose,
        mesh=mesh,
        in_specs=placed,
        out_specs=(P("rep", "fsdp", None), P("fsdp", "rep", None, None, None)),
        check_vma=False,
    )
```
